128 devices in a mesh: lon: 16 (over x_lo, z, core), lat: 8 (over y, x_hi).
Axes of the slice: x: 4 (x_hi: 2, x_lo: 2; x = x_hi * 2 + x_lo), y: 4, z: 4, core: 2. Of those that a mesh axis runs over, the one named last changes fastest.
Arguments:
- height: float32 [1, 1152, 4096], P(None, 'lat', 'lon'), may hold values from -6 to 6
- response: float32 [640], replicated, may hold values from 0.25 to 4
Outputs:
- loading: float32 [1, 1152, 4096], P(None, 'lat', 'lon')
The draws below stay inside these ranges and needn't reach their ends.
All inputs are finite; a program needn't handle non-finite values.
Results may differ from the reference program's by a relative error of at most 0.00085.
Values sent between devices are 32-bit elements; how exact they have to be, the bound alone decides.
A program may use at most 64 MiB of HBM per device.

```python
import math
import jax
import jax.numpy as jnp
from jax import lax

NLAT = 1152
NLON = 4096
MODES = 640
FIELDS = 1


def block_scale(stream_key, shape, split, least, high):
    loudness = 1.0
    for dim, parts in split:
        draws = jax.random.uniform(jax.random.fold_in(jax.random.fold_in(stream_key, 6), dim), (parts,), jnp.float32, least / len(split), high / len(split))
        loudness = loudness * jnp.repeat(jnp.exp(draws), shape[dim] // parts).reshape((-1,) + (1,) * (len(shape) - 1 - dim))
    return loudness


def centred(key, extent, width, reach, split=(), held_as=jnp.bfloat16):
    array = jax.random.normal(key, extent, jnp.float32) * width
    if len(split) > 0:
        array = block_scale(key, extent, split, -0.22, 0.18) * array
    return jnp.clip(array, min=-reach, max=reach).astype(held_as)


def setup_inputs(seed: int = 0) -> dict:
    splits = jax.random.split(jax.random.key(seed), 3)
    return {
        "height": centred(splits[0], (FIELDS, NLAT, NLON), 1.0, 6.0, ((1, 8), (2, 16)), jnp.float32),
        "response": jnp.clip(jnp.exp(jax.random.uniform(splits[1], (MODES,), jnp.float32, math.log(0.25), math.log(4.0))), 0.25, 4.0),
    }


block_degrees = 64
rescale_every = 8
highest = lax.Precision.HIGHEST

def colatitude_parts(latitudes):
    colatitude = (latitudes.astype(jnp.float32) + 0.5) * (jnp.pi / NLAT)
    sines = jnp.sin(colatitude)
    return (jnp.cos(colatitude), sines, sines * (jnp.pi / NLAT))

def legendre_sweep(cosines, sines, orders, consume, initial):
    order_float = orders.astype(jnp.float32)
    log_start = 0.5 * (lax.lgamma(order_float + 1.5) - lax.lgamma(order_float + 1.0) - lax.lgamma(jnp.full_like(order_float, 1.5))) - 0.5 * jnp.log(4.0 * jnp.pi)
    log_scale = log_start[:, None] + order_float[:, None] * jnp.log(sines)[None, :]
    zero_field = jnp.zeros(log_scale.shape, jnp.float32)

    def one_block(block_index, carried):
        earlier, latest, log_scale, running = carried
        first_degree = (block_index * block_degrees).astype(jnp.int32)
        factor = jnp.exp(log_scale)
        layers = []
        for offset in range(block_degrees):
            degree = first_degree + offset
            started = degree > orders
            starting = degree == orders
            degree_float = degree.astype(jnp.float32)
            lower_float = degree_float - 1.0
            square_gap = jnp.where(started, degree_float * degree_float - order_float * order_float, 1.0)
            growth = jnp.sqrt(jnp.where(started, (4.0 * degree_float * degree_float - 1.0) / square_gap, 0.0))
            damping = jnp.sqrt(jnp.where(started, (lower_float * lower_float - order_float * order_float) / jnp.maximum(4.0 * lower_float * lower_float - 1.0, 1.0), 0.0))
            current = jnp.where(starting[:, None], 1.0, growth[:, None] * (cosines[None, :] * latest - damping[:, None] * earlier))
            layers.append(current * factor)
            earlier, latest = (latest, current)
            if (offset + 1) % rescale_every == 0:
                largest = jnp.maximum(jnp.maximum(jnp.abs(earlier), jnp.abs(latest)), 1.0)
                earlier = earlier / largest
                latest = latest / largest
                log_scale = log_scale + jnp.log(largest)
                factor = jnp.exp(log_scale)
        legendre = jnp.stack(layers)
        return (earlier, latest, log_scale, consume(running, legendre, first_degree))
    carried = (zero_field, zero_field, log_scale, initial)
    carried = lax.fori_loop(0, MODES // block_degrees, one_block, carried)
    return carried[3]

def analyse(spectrum, latitudes, orders):
    cosines, sines, weights = colatitude_parts(latitudes)
    weighted = spectrum * weights

    def consume(coefficients, legendre, first_degree):
        block_terms = jnp.einsum('lmj,mcfj->lmcf', legendre, weighted, precision=highest)
        return lax.dynamic_update_slice_in_dim(coefficients, block_terms, first_degree, 0)
    initial = jnp.zeros((MODES,) + spectrum.shape[:3], jnp.float32)
    return legendre_sweep(cosines, sines, orders, consume, initial)

def synthesise(scaled, latitudes, orders):
    cosines, sines = colatitude_parts(latitudes)[:2]

    def consume(running, legendre, first_degree):
        scaled_block = lax.dynamic_slice_in_dim(scaled, first_degree, block_degrees, 0)
        return running + jnp.einsum('lmj,lmcf->mcfj', legendre, scaled_block, precision=highest)
    initial = jnp.zeros(scaled.shape[1:] + (latitudes.shape[0],), jnp.float32)
    return legendre_sweep(cosines, sines, orders, consume, initial)

def reference(height, response):
    transform = jnp.fft.rfft(height, axis=2)[:, :, :MODES] * (2.0 * jnp.pi / NLON)
    spectral_parts = jnp.stack([jnp.real(transform), jnp.imag(transform)], axis=0)
    spectral_parts = jnp.transpose(spectral_parts, (3, 0, 1, 2)).astype(jnp.float32)
    all_rows = jnp.arange(NLAT, dtype=jnp.int32)
    groups = spectral_parts.reshape((MODES // block_degrees, block_degrees) + spectral_parts.shape[1:])

    def one_group(group_pair):
        block_index, group_spectrum = group_pair
        orders = block_index * block_degrees + jnp.arange(block_degrees, dtype=jnp.int32)
        coefficients = analyse(group_spectrum, all_rows, orders)
        scaled = coefficients * response[:, None, None, None]
        return synthesise(scaled, all_rows, orders)
    synthesis = lax.map(one_group, (jnp.arange(MODES // block_degrees, dtype=jnp.int32), groups))
    synthesis = synthesis.reshape((MODES,) + synthesis.shape[2:])
    complex_parts = jnp.transpose(synthesis[:, 0] + 1j * synthesis[:, 1], (1, 2, 0))
    padded = jnp.pad(complex_parts, ((0, 0), (0, 0), (0, NLON // 2 + 1 - MODES)))
    loading = jnp.fft.irfft(padded, n=NLON, axis=2) * NLON
    return loading.astype(jnp.float32)
```

```python
import math

import jax
import jax.numpy as jnp
import numpy as np
from jax import lax
from jax.experimental import pallas as pl
from jax.experimental.pallas import tpu as pltpu
from jax.sharding import PartitionSpec as P

NLAT = 1152
NLON = 4096
MODES = 640
LON = 16
LAT = 8
DEV = LON * LAT
ROWS = NLAT // DEV
CELLS = NLON // LON
SLOTS = MODES // DEV
HALF = DEV // 2
STARTS = [sum(MODES - DEV * t for t in range(i)) for i in range(SLOTS)]
TALL = sum(MODES - DEV * t for t in range(SLOTS))
WIDE = 640
bf16 = jnp.bfloat16
f32 = jnp.float32


def constants():
    t = np.arange(CELLS)
    table = np.zeros((2 * CELLS, 128))
    for g in range(LAT):
        for i in range(SLOTS):
            angle = 2 * np.pi * ((g + LAT * i) * t % CELLS) / CELLS
            column = (g * SLOTS + i) * 2
            table[:CELLS, column] = np.cos(angle)
            table[CELLS:, column] = np.sin(angle)
            table[:CELLS, column + 1] = -np.sin(angle)
            table[CELLS:, column + 1] = np.cos(angle)
    high = table.astype(np.float32).astype(bf16)
    low = (table - high.astype(np.float64)).astype(np.float32).astype(bf16)
    angle = 2 * np.pi * np.arange(LON)[:, None] * t[None, :] / NLON
    twiddle = np.stack([np.cos(angle), np.sin(angle)]).astype(np.float32)
    geometry = np.zeros((4, 8, 128), np.float32)
    for chunk in range(5):
        for lane in range(128):
            r = 2 * chunk + lane // HALF
            if r < ROWS:
                theta = np.pi * (ROWS * (lane % HALF) + r + 0.5) / NLAT
                log_sine = np.log2(np.sin(theta))
                coarse = np.round(log_sine * 1024) / 1024
                geometry[:, chunk, lane] = np.cos(theta), coarse, log_sine - coarse, 1.0
    weights = np.zeros((HALF, 128), np.float32)
    for r in range(ROWS):
        theta = np.pi * (ROWS * np.arange(HALF) + r + 0.5) / NLAT
        cell = np.sin(theta) * (np.pi / NLAT) * (2 * np.pi / NLON)
        weights[:, 10 * r : 10 * r + 10] = cell[:, None]
    first = [
        (0.5 * (math.lgamma(m + 1.5) - math.lgamma(1.5) - math.lgamma(m + 1.0)) - 0.5 * math.log(4 * math.pi))
        / math.log(2)
        for m in range(MODES)
    ]
    return high, low, twiddle, geometry, weights, np.asarray(first, np.float32)


def split(x):
    high = x.astype(bf16)
    return high, (x - high.astype(f32)).astype(bf16)


def cosine(n):
    return math.cos(math.pi * (n % 16) / 8)


def sine(n):
    return math.sin(math.pi * (n % 16) / 8)


def combine(terms):
    total = None
    for value, factor in terms:
        if abs(factor) < 1e-9:
            continue
        if abs(factor - 1) < 1e-9:
            term, negative = value, False
        elif abs(factor + 1) < 1e-9:
            term, negative = value, True
        else:
            term, negative = value * factor, False
        if total is None:
            total = -term if negative else term
        else:
            total = total - term if negative else total + term
    return 0.0 if total is None else total


def kernel(
    h_ref, resp_ref, thi_ref, tlo_ref, tw_ref, geo_ref, wt_ref, lc_ref, o_ref,
    send_a, recv_a, zs, osc, send_b, recv_b, coef_a, coef_c, tall, phi, plo, fold, send_c, recv_c, vs, send_d, recv_d,
    ssem, rsem,
):
    lon = lax.axis_index("lon")
    lat = lax.axis_index("lat")
    me = lat * LON + lon
    south = lat // (LAT // 2)
    barrier = pltpu.get_barrier_semaphore()

    def peer(p):
        return {"lat": p // LON, "lon": p % LON}

    def place(p):
        return jnp.where(p < HALF, p, DEV + HALF - 1 - p)

    def greet(step, carry):
        pl.semaphore_signal(barrier, inc=1, device_id=peer(lax.rem(me + step, DEV)))
        return carry

    lax.fori_loop(1, DEV, greet, 0)

    def stage(block, carry):
        for r in range(ROWS):
            source = jnp.where(south == 1, ROWS - 1 - r, r)
            send_a[block, r : r + 1, :] = h_ref[pl.ds(ROWS * block + source, 1), :]
        return carry

    lax.fori_loop(0, LON, stage, 0)

    for i in range(SLOTS):
        def coefficients(block, carry, i=i):
            row = block * 32
            m = (DEV * i + me).astype(f32)
            k = (row + lax.broadcasted_iota(jnp.int32, (32, 128), 0)).astype(f32)
            k1 = k + 1.0
            l2 = 2.0 * (m + k1)
            squared = (l2 * l2 - 1.0) / (k1 * (2.0 * m + k1))
            below = l2 - 2.0
            ratio = k * (2.0 * m + k) / jnp.maximum(below * below - 1.0, 1.0)
            start = pl.multiple_of(STARTS[i] + row, 8)
            coef_a[pl.ds(start, 32), :] = jnp.sqrt(squared)
            coef_c[pl.ds(start, 32), :] = jnp.sqrt(squared * ratio)
            return carry

        lax.fori_loop(0, (MODES - DEV * i) // 32, coefficients, 0)

    pl.semaphore_wait(barrier, DEV - 1)

    def exchange_lon(send, recv, which):
        def go(step, carry):
            p = lax.rem(lon + step, LON)
            pltpu.make_async_remote_copy(
                send.at[p], recv.at[lon], ssem.at[which], rsem.at[which], device_id={"lat": lat, "lon": p}
            ).start()
            return carry

        lax.fori_loop(1, LON, go, 0)
        recv[lon] = send[lon]

    def finish(send, recv, which, count):
        every = pltpu.make_async_remote_copy(
            send.at[pl.ds(0, count)], recv.at[pl.ds(0, count)], ssem.at[which], rsem.at[which],
            device_id=peer(lax.rem(me + 1, DEV)),
        )
        every.wait_send()
        every.wait_recv()

    exchange_lon(send_a, recv_a, 0)

    x = geo_ref[0]
    state = []
    for i in range(SLOTS):
        m = (DEV * i + me).astype(f32)
        coarse = m * geo_ref[1]
        fine = m * geo_ref[2] + lc_ref[DEV * i + me]
        count = jnp.maximum(jnp.ceil((-84.0 - (coarse + fine)) * (1.0 / 64.0)), 0.0)
        value = jnp.exp2((coarse + 64.0 * count) + fine) * geo_ref[3]
        state.append((jnp.zeros_like(value), value, count))

    for section in range(SLOTS):
        active = SLOTS - section

        def steps(block, carry, section=section, active=active):
            new = []
            for i in range(active):
                earlier, latest, count = carry[i]
                base = STARTS[i] + section * DEV
                row = pl.multiple_of(base + block * 8, 8)
                a8 = coef_a[pl.ds(row, 8), :]
                c8 = coef_c[pl.ds(row, 8), :]
                seen = jnp.where(count == 0.0, 1.0, 0.0)
                for u in range(8):
                    tall[pl.ds(pl.multiple_of((row + u) * 8, 8), 8), :] = latest * seen
                    following = (a8[u : u + 1, :] * x) * latest - c8[u : u + 1, :] * earlier
                    earlier, latest = latest, following
                large = jnp.logical_and(jnp.abs(latest) > 2.0**-20, count > 0.0)
                factor = jnp.where(large, 2.0**-64, 1.0)
                new.append((earlier * factor, latest * factor, count - jnp.where(large, 1.0, 0.0)))
            return tuple(new)

        state = list(lax.fori_loop(0, DEV // 8, steps, tuple(state[:active])))

    def halves(block, carry):
        row = pl.multiple_of(block * 16, 16)
        for j in range(5):
            value = tall[pl.ds(row * 8 + j, 16, stride=8), :]
            high, low = split(value)
            phi[pl.ds(row, 16), j * 128 : (j + 1) * 128] = high
            plo[pl.ds(row, 16), j * 128 : (j + 1) * 128] = low
        return carry

    lax.fori_loop(0, TALL // 16, halves, 0)

    finish(send_a, recv_a, 0, LON - 1)

    for side in range(2):
        lanes = slice(side * 128, side * 128 + 128)
        d = [recv_a[b, :, lanes] for b in range(LON)]
        even = {b: d[b] + d[16 - b] for b in range(1, 8)}
        odd = {b: d[b] - d[16 - b] for b in range(1, 8)}
        real = [None] * 9
        imag = [None] * 9
        for rho in range(5):
            a = combine(
                [(d[0], 1.0), (d[8], 1.0 - 2.0 * (rho % 2))] + [(even[b], cosine(rho * b)) for b in (2, 4, 6)]
            )
            b_ = combine([(even[b], cosine(rho * b)) for b in (1, 3, 5, 7)])
            e = combine([(odd[b], -sine(rho * b)) for b in (2, 4, 6)])
            c = combine([(odd[b], -sine(rho * b)) for b in (1, 3, 5, 7)])
            real[rho], real[8 - rho] = a + b_, a - b_
            imag[rho], imag[8 - rho] = c + e, c - e
        for rho in range(LON):
            tc = tw_ref[0, rho : rho + 1, lanes]
            ts = tw_ref[1, rho : rho + 1, lanes]
            if rho % 8 == 0:
                zre, zim = real[rho] * tc, -(real[rho] * ts)
            elif rho < 8:
                zre, zim = real[rho] * tc + imag[rho] * ts, imag[rho] * tc - real[rho] * ts
            else:
                yre, yim = real[16 - rho], imag[16 - rho]
                zre, zim = yre * tc - yim * ts, -(yim * tc) - yre * ts
            zs[rho, 0:ROWS, lanes] = zre
            zs[rho, 0:ROWS, CELLS + side * 128 : CELLS + side * 128 + 128] = zim

    zh, zl = split(zs[...].reshape(LON * 16, 2 * CELLS))
    thi = thi_ref[...]
    tlo = tlo_ref[...]
    dims = (((1,), (0,)), ((), ()))
    osc[...] = (
        lax.dot_general(zh, thi, dims, preferred_element_type=f32)
        + lax.dot_general(zl, thi, dims, preferred_element_type=f32)
        + lax.dot_general(zh, tlo, dims, preferred_element_type=f32)
    )

    lane = lax.broadcasted_iota(jnp.int32, (LON, 128), 1)
    packed = [jnp.zeros((LON, 128), f32) for _ in range(LAT)]
    for r in range(ROWS):
        value = osc[pl.ds(r, LON, stride=16), :]
        mine = jnp.logical_and(lane >= 10 * r, lane < 10 * r + 10)
        for g in range(LAT):
            shift = (10 * (r - g)) % 128
            moved = pltpu.roll(value, shift, axis=1) if shift else value
            packed[g] = jnp.where(mine, moved, packed[g])
    for g in range(LAT):
        send_b[g * LON : (g + 1) * LON, 0, :] = packed[g]

    def exchange_all(send, recv, which, source, target):
        def go(step, carry):
            p = lax.rem(me + step, DEV)
            pltpu.make_async_remote_copy(
                send.at[source(p)], recv.at[target], ssem.at[which], rsem.at[which], device_id=peer(p)
            ).start()
            return carry

        lax.fori_loop(1, DEV, go, 0)
        recv[target] = send[source(me)]

    exchange_all(send_b, recv_b, 1, lambda p: p, place(me))

    wide = jnp.concatenate([resp_ref[...], jnp.zeros((1, MODES), f32)], axis=1)
    shifted = pltpu.roll(jnp.broadcast_to(wide, (8, 2 * MODES)), lax.rem(2 * MODES - me, 2 * MODES), axis=1)
    response = jnp.concatenate([shifted[:1, DEV * i : MODES] for i in range(SLOTS)], axis=1)
    first = jnp.where(jnp.logical_and(lax.broadcasted_iota(jnp.int32, (1, TALL), 1) < MODES, me == 0), 1.0, 2.0)
    response = response * first
    row = lax.broadcasted_iota(jnp.int32, (32, TALL), 0)
    column = lax.broadcasted_iota(jnp.int32, (32, TALL), 1)
    slot = jnp.zeros((32, TALL), jnp.int32)
    for i in range(1, SLOTS):
        slot = slot + jnp.where(column >= STARTS[i], 1, 0)
    wanted = 2 * slot + 16 * (column & 1)
    keep = jnp.logical_or(row == wanted, row == wanted + 1)
    gain = jnp.where(keep, response, 0.0)

    finish(send_b, recv_b, 1, DEV - 1)

    north = recv_b[0:HALF, 0, :]
    southern = recv_b[HALF:DEV, 0, :]
    weights = wt_ref[...]
    folded = jnp.concatenate([(north + southern) * weights, (north - southern) * weights], axis=0)
    fold[...] = folded.T
    left = lax.broadcasted_iota(jnp.int32, (10, 128), 1) < HALF
    evens = []
    odds = []
    for j in range(5):
        first_row = fold[20 * j : 20 * j + 10, :]
        if j < 4:
            second_row = fold[20 * j + 10 : 20 * j + 20, :]
        else:
            second_row = jnp.zeros((10, 128), f32)
        evens.append(jnp.where(left, first_row, pltpu.roll(second_row, HALF, axis=1)))
        odds.append(jnp.where(left, pltpu.roll(first_row, HALF, axis=1), second_row))
    pad = jnp.zeros((6, WIDE), f32)
    lhs = jnp.concatenate([jnp.concatenate(evens, axis=1), pad, jnp.concatenate(odds, axis=1), pad], axis=0)
    lh, ll = split(lhs)
    nt = (((1,), (1,)), ((), ()))
    coefficients_ = (
        lax.dot_general(lh, phi[...], nt, preferred_element_type=f32)
        + lax.dot_general(ll, phi[...], nt, preferred_element_type=f32)
        + lax.dot_general(lh, plo[...], nt, preferred_element_type=f32)
    )
    sh, sl = split(coefficients_ * gain)
    synthesis = (
        lax.dot_general(sh, phi[...], dims, preferred_element_type=f32)
        + lax.dot_general(sl, phi[...], dims, preferred_element_type=f32)
        + lax.dot_general(sh, plo[...], dims, preferred_element_type=f32)
    )
    fold[...] = jnp.zeros((128, 128), f32)
    for j in range(5):
        e = synthesis[0:10, j * 128 : (j + 1) * 128]
        o = synthesis[16:26, j * 128 : (j + 1) * 128]
        n, s = e + o, e - o
        fold[20 * j : 20 * j + 10, :] = jnp.where(left, n, pltpu.roll(s, HALF, axis=1))
        if j < 4:
            fold[20 * j + 10 : 20 * j + 20, :] = jnp.where(left, pltpu.roll(n, HALF, axis=1), s)
    send_c[:, 0, :] = fold[...].T

    exchange_all(send_c, recv_c, 2, place, me)
    finish(send_c, recv_c, 2, DEV - 1)

    pieces = [recv_c[g * LON : (g + 1) * LON, 0, :] for g in range(LAT)]
    gathered = []
    for r in range(ROWS):
        value = jnp.zeros((LON, 128), f32)
        for g in range(LAT):
            mine = jnp.logical_and(lane >= 10 * g, lane < 10 * g + 10)
            shift = (10 * (g - r)) % 128
            moved = pltpu.roll(pieces[g], shift, axis=1) if shift else pieces[g]
            value = jnp.where(mine, moved, value)
        gathered.append(value)
    gh, gl = split(jnp.concatenate(gathered, axis=0))
    inverse = (
        lax.dot_general(gh, thi, nt, preferred_element_type=f32)
        + lax.dot_general(gl, thi, nt, preferred_element_type=f32)
        + lax.dot_general(gh, tlo, nt, preferred_element_type=f32)
    )
    for c in range(4):
        vs[c] = inverse[:, c * 128 : (c + 1) * 128]

    for side in range(2):
        lanes = slice(side * 128, side * 128 + 128)
        real = []
        imag = []
        for rho in range(LON):
            tc = tw_ref[0, rho : rho + 1, lanes]
            ts = tw_ref[1, rho : rho + 1, lanes]
            vre = vs[side, pl.ds(rho, ROWS, stride=16), :]
            vim = vs[2 + side, pl.ds(rho, ROWS, stride=16), :]
            real.append(vre * tc - vim * ts)
            imag.append(None if rho % 8 == 0 else vre * ts + vim * tc)
        ure = {rho: real[rho] + real[16 - rho] for rho in range(1, 8)}
        uim = {rho: imag[rho] - imag[16 - rho] for rho in range(1, 8)}
        for b in range(5):
            ge = combine(
                [(real[0], 1.0), (real[8], 1.0 - 2.0 * (b % 2))] + [(ure[q], cosine(q * b)) for q in (2, 4, 6)]
            )
            go = combine([(ure[q], cosine(q * b)) for q in (1, 3, 5, 7)])
            he = combine([(uim[q], sine(q * b)) for q in (2, 4, 6)])
            ho = combine([(uim[q], sine(q * b)) for q in (1, 3, 5, 7)])
            send_d[b, :, lanes] = (ge + go) - (he + ho)
            if b > 0:
                send_d[16 - b, :, lanes] = (ge + go) + (he + ho)
            if b < 4:
                send_d[8 - b, :, lanes] = (ge - go) - (ho - he)
                if b > 0:
                    send_d[8 + b, :, lanes] = (ge - go) + (ho - he)

    exchange_lon(send_d, recv_d, 3)
    finish(send_d, recv_d, 3, LON - 1)

    def unstage(block, carry):
        for r in range(ROWS):
            target = jnp.where(south == 1, ROWS - 1 - r, r)
            o_ref[pl.ds(ROWS * block + target, 1), :] = recv_d[block, r : r + 1, :]
        return carry

    lax.fori_loop(0, LON, unstage, 0)


def shards(height, response):
    high, low, twiddle, geometry, weights, first = constants()
    vmem = pl.BlockSpec(memory_space=pltpu.VMEM)
    smem = pl.BlockSpec(memory_space=pltpu.SMEM)
    blocks = pltpu.VMEM((LON, ROWS, CELLS), f32)
    rows = pltpu.VMEM((DEV, 1, 128), f32)
    out = pl.pallas_call(
        kernel,
        out_shape=jax.ShapeDtypeStruct((NLAT // LAT, CELLS), f32),
        in_specs=[vmem] * 7 + [smem],
        out_specs=vmem,
        scratch_shapes=[
            blocks,
            blocks,
            pltpu.VMEM((LON, 16, 2 * CELLS), f32),
            pltpu.VMEM((LON * 16, 128), f32),
            rows,
            rows,
            pltpu.VMEM((TALL, 128), f32),
            pltpu.VMEM((TALL, 128), f32),
            pltpu.VMEM((TALL * 8, 128), f32),
            pltpu.VMEM((TALL, WIDE), bf16),
            pltpu.VMEM((TALL, WIDE), bf16),
            pltpu.VMEM((128, 128), f32),
            rows,
            rows,
            pltpu.VMEM((4, ROWS * LON, 128), f32),
            blocks,
            blocks,
            pltpu.SemaphoreType.DMA((4,)),
            pltpu.SemaphoreType.DMA((4,)),
        ],
        compiler_params=pltpu.CompilerParams(
            collective_id=0, has_side_effects=True, vmem_limit_bytes=60 * 1024 * 1024
        ),
    )(
        height.reshape(NLAT // LAT, CELLS),
        response.reshape(1, MODES),
        jnp.asarray(high),
        jnp.asarray(low),
        jnp.asarray(twiddle),
        jnp.asarray(geometry),
        jnp.asarray(weights),
        jnp.asarray(first),
    )
    return out.reshape(height.shape)


def solution(mesh):
    placed = (P(None, "lat", "lon"), P())
    return jax.shard_map(
        shards, mesh=mesh, in_specs=placed, out_specs=P(None, "lat", "lon"), check_vma=False
    )
```

```python
import math

import jax
import jax.numpy as jnp
import numpy as np
from jax import lax
from jax.experimental import pallas as pl
from jax.experimental.pallas import tpu as pltpu
from jax.sharding import PartitionSpec as P

NLAT = 1152
NLON = 4096
MODES = 640
LON = 16
LAT = 8
DEV = LON * LAT
ROWS = NLAT // DEV
CELLS = NLON // LON
SLOTS = MODES // DEV
HALF = DEV // 2
STARTS = [sum(MODES - DEV * t for t in range(i)) for i in range(SLOTS)]
TALL = sum(MODES - DEV * t for t in range(SLOTS))
WIDE = 640
HOPS = (0, 1, 2, 1)
FAR = sorted(
    [(dy, dx, dz, dc) for dy in range(4) for dx in range(4) for dz in range(4) for dc in range(2)],
    key=lambda o: (-HOPS[o[0]] - HOPS[o[1]] - HOPS[o[2]], -o[3]),
)[: DEV - 1]
FAR_LON = sorted(
    [(dx, dz, dc) for dx in range(2) for dz in range(4) for dc in range(2)],
    key=lambda o: (-o[0] - HOPS[o[1]], -o[2]),
)[: LON - 1]
bf16 = jnp.bfloat16
f32 = jnp.float32


def constants():
    t = np.arange(CELLS)
    table = np.zeros((2 * CELLS, 128))
    for g in range(LAT):
        for i in range(SLOTS):
            angle = 2 * np.pi * ((g + LAT * i) * t % CELLS) / CELLS
            column = (g * SLOTS + i) * 2
            table[:CELLS, column] = np.cos(angle)
            table[CELLS:, column] = np.sin(angle)
            table[:CELLS, column + 1] = -np.sin(angle)
            table[CELLS:, column + 1] = np.cos(angle)
    high = table.astype(np.float32).astype(bf16)
    low = (table - high.astype(np.float64)).astype(np.float32).astype(bf16)
    angle = 2 * np.pi * np.arange(LON)[:, None] * t[None, :] / NLON
    twiddle = np.stack([np.cos(angle), np.sin(angle)]).astype(np.float32)
    geometry = np.zeros((4, 8, 128), np.float32)
    for chunk in range(5):
        for lane in range(128):
            r = 2 * chunk + lane // HALF
            if r < ROWS:
                theta = np.pi * (ROWS * (lane % HALF) + r + 0.5) / NLAT
                log_sine = np.log2(np.sin(theta))
                coarse = np.round(log_sine * 1024) / 1024
                geometry[:, chunk, lane] = np.cos(theta), coarse, log_sine - coarse, 1.0
    weights = np.zeros((HALF, 128), np.float32)
    for r in range(ROWS):
        theta = np.pi * (ROWS * np.arange(HALF) + r + 0.5) / NLAT
        cell = np.sin(theta) * (np.pi / NLAT) * (2 * np.pi / NLON)
        weights[:, 10 * r : 10 * r + 10] = cell[:, None]
    first = [
        (0.5 * (math.lgamma(m + 1.5) - math.lgamma(1.5) - math.lgamma(m + 1.0)) - 0.5 * math.log(4 * math.pi))
        / math.log(2)
        for m in range(MODES)
    ]
    return high, low, twiddle, geometry, weights, np.asarray(first, np.float32)


def split(x):
    high = x.astype(bf16)
    return high, (x - high.astype(f32)).astype(bf16)


def cosine(n):
    return math.cos(math.pi * (n % 16) / 8)


def sine(n):
    return math.sin(math.pi * (n % 16) / 8)


def combine(terms):
    total = None
    for value, factor in terms:
        if abs(factor) < 1e-9:
            continue
        if abs(factor - 1) < 1e-9:
            term, negative = value, False
        elif abs(factor + 1) < 1e-9:
            term, negative = value, True
        else:
            term, negative = value * factor, False
        if total is None:
            total = -term if negative else term
        else:
            total = total - term if negative else total + term
    return 0.0 if total is None else total


def kernel(
    h_hbm, resp_hbm, thi_hbm, tlo_hbm, tw_hbm, geo_hbm, wt_hbm, lc_ref, o_ref,
    h_ref, resp_ref, thi_ref, tlo_ref, tw_ref, geo_ref, wt_ref,
    send_a, recv_a, zs, osc, send_b, recv_b, coef_a, coef_c, tall, phi, plo, fold, send_c, recv_c, vs, send_d, recv_d,
    ssem, rsem, lsem,
):
    loads = [
        pltpu.make_async_copy(source, target, lsem.at[n])
        for n, (source, target) in enumerate(
            [
                (h_hbm, h_ref),
                (geo_hbm, geo_ref),
                (tw_hbm, tw_ref),
                (thi_hbm, thi_ref),
                (tlo_hbm, tlo_ref),
                (wt_hbm, wt_ref),
                (resp_hbm, resp_ref.at[pl.ds(0, SLOTS)]),
            ]
        )
    ]
    resp_ref[...] = jnp.zeros((8, 128), f32)
    for load in loads:
        load.start()
    lon = lax.axis_index("lon")
    lat = lax.axis_index("lat")
    me = lat * LON + lon
    south = lat // (LAT // 2)
    barrier = pltpu.get_barrier_semaphore()

    y, z, core = lat // 2, (lon // 2) % 4, lon % 2
    x_low = lon // 8
    x_all = (lat % 2) * 2 + x_low
    at_y = [((y + d) % 4) * 2 for d in range(4)]
    at_x = [(x_all + d) % 4 for d in range(4)]
    at_x = [(v // 2, (v % 2) * 8) for v in at_x]
    at_low = [((x_low + d) % 2) * 8 for d in range(2)]
    at_z = [((z + d) % 4) * 2 for d in range(4)]
    at_core = [core, 1 - core]
    everyone = [(at_y[dy] + at_x[dx][0], at_x[dx][1] + at_z[dz] + at_core[dc]) for dy, dx, dz, dc in FAR]
    row_peers = [at_low[dx] + at_z[dz] + at_core[dc] for dx, dz, dc in FAR_LON]

    def place(a, b):
        p = a * LON + b
        return jnp.where(a < LAT // 2, p, DEV + HALF - 1 - p)

    for a, b in everyone:
        pl.semaphore_signal(barrier, inc=1, device_id={"lat": a, "lon": b})

    loads[0].wait()

    def stage(block, carry):
        for r in range(ROWS):
            source = jnp.where(south == 1, ROWS - 1 - r, r)
            line = h_ref[pl.ds(ROWS * block + source, 1), :]
            send_a[block, r] = line[:, :128]
            send_a[block, ROWS + r] = line[:, 128:]
        return carry

    lax.fori_loop(0, LON, stage, 0)

    for i in range(SLOTS):
        def coefficients(block, carry, i=i):
            row = block * 32
            m = (DEV * i + me).astype(f32)
            k = (row + lax.broadcasted_iota(jnp.int32, (32, 128), 0)).astype(f32)
            k1 = k + 1.0
            l2 = 2.0 * (m + k1)
            squared = (l2 * l2 - 1.0) / (k1 * (2.0 * m + k1))
            below = l2 - 2.0
            ratio = k * (2.0 * m + k) / jnp.maximum(below * below - 1.0, 1.0)
            start = pl.multiple_of(STARTS[i] + row, 8)
            coef_a[pl.ds(start, 32), :] = jnp.sqrt(squared)
            coef_c[pl.ds(start, 32), :] = jnp.sqrt(squared * ratio)
            return carry

        lax.fori_loop(0, (MODES - DEV * i) // 32, coefficients, 0)

    loads[1].wait()
    x = geo_ref[0]
    state = []
    for i in range(SLOTS):
        m = (DEV * i + me).astype(f32)
        coarse = m * geo_ref[1]
        fine = m * geo_ref[2] + lc_ref[DEV * i + me]
        count = jnp.maximum(jnp.ceil((-84.0 - (coarse + fine)) * (1.0 / 64.0)), 0.0)
        value = jnp.exp2((coarse + 64.0 * count) + fine) * geo_ref[3]
        state.append((jnp.zeros_like(value), value, count))

    for section in range(SLOTS):
        active = SLOTS - section

        def steps(block, carry, section=section, active=active):
            new = []
            for i in range(active):
                earlier, latest, count = carry[i]
                base = STARTS[i] + section * DEV
                row = pl.multiple_of(base + block * 8, 8)
                a8 = coef_a[pl.ds(row, 8), :]
                c8 = coef_c[pl.ds(row, 8), :]
                seen = jnp.where(count == 0.0, 1.0, 0.0)
                for u in range(8):
                    tall[pl.ds(pl.multiple_of((row + u) * 8, 8), 8), :] = latest * seen
                    following = (a8[u : u + 1, :] * x) * latest - c8[u : u + 1, :] * earlier
                    earlier, latest = latest, following
                large = jnp.logical_and(jnp.abs(latest) > 2.0**-20, count > 0.0)
                factor = jnp.where(large, 2.0**-64, 1.0)
                new.append((earlier * factor, latest * factor, count - jnp.where(large, 1.0, 0.0)))
            return tuple(new)

        state = list(lax.fori_loop(0, DEV // 8, steps, tuple(state[:active])))

    pl.semaphore_wait(barrier, DEV - 1)

    def exchange_lon(send, recv, which):
        for b in row_peers:
            pltpu.make_async_remote_copy(
                send.at[b], recv.at[lon], ssem.at[which], rsem.at[which], device_id={"lat": lat, "lon": b}
            ).start()
        recv[lon] = send[lon]

    def finish(send, recv, which, count):
        every = pltpu.make_async_remote_copy(
            send.at[pl.ds(0, count)], recv.at[pl.ds(0, count)], ssem.at[which], rsem.at[which],
            device_id={"lat": lat, "lon": row_peers[0]},
        )
        every.wait_send()
        every.wait_recv()

    exchange_lon(send_a, recv_a, 0)

    def halves(block, carry):
        row = pl.multiple_of(block * 16, 16)
        for j in range(5):
            value = tall[pl.ds(row * 8 + j, 16, stride=8), :]
            high, low = split(value)
            phi[pl.ds(row, 16), j * 128 : (j + 1) * 128] = high
            plo[pl.ds(row, 16), j * 128 : (j + 1) * 128] = low
        return carry

    lax.fori_loop(0, TALL // 16, halves, 0)

    finish(send_a, recv_a, 0, LON - 1)

    loads[2].wait()
    for side in range(2):
        lanes = slice(side * 128, side * 128 + 128)
        d = [recv_a[b, side * ROWS : side * ROWS + ROWS, 0, :] for b in range(LON)]
        even = {b: d[b] + d[16 - b] for b in range(1, 8)}
        odd = {b: d[b] - d[16 - b] for b in range(1, 8)}
        real = [None] * 9
        imag = [None] * 9
        for rho in range(5):
            a = combine(
                [(d[0], 1.0), (d[8], 1.0 - 2.0 * (rho % 2))] + [(even[b], cosine(rho * b)) for b in (2, 4, 6)]
            )
            b_ = combine([(even[b], cosine(rho * b)) for b in (1, 3, 5, 7)])
            e = combine([(odd[b], -sine(rho * b)) for b in (2, 4, 6)])
            c = combine([(odd[b], -sine(rho * b)) for b in (1, 3, 5, 7)])
            real[rho], real[8 - rho] = a + b_, a - b_
            imag[rho], imag[8 - rho] = c + e, c - e
        for rho in range(LON):
            tc = tw_ref[0, rho : rho + 1, lanes]
            ts = tw_ref[1, rho : rho + 1, lanes]
            if rho % 8 == 0:
                zre, zim = real[rho] * tc, -(real[rho] * ts)
            elif rho < 8:
                zre, zim = real[rho] * tc + imag[rho] * ts, imag[rho] * tc - real[rho] * ts
            else:
                yre, yim = real[16 - rho], imag[16 - rho]
                zre, zim = yre * tc - yim * ts, -(yim * tc) - yre * ts
            zs[rho, 0:ROWS, lanes] = zre
            zs[rho, 0:ROWS, CELLS + side * 128 : CELLS + side * 128 + 128] = zim

    loads[3].wait()
    loads[4].wait()
    zh, zl = split(zs[...].reshape(LON * 16, 2 * CELLS))
    thi = thi_ref[...]
    tlo = tlo_ref[...]
    nn = (((1,), (0,)), ((), ()))
    nt = (((1,), (1,)), ((), ()))

    def product(high, low, other_high, other_low, dims):
        count = high.shape[0]
        both = lax.dot_general(jnp.concatenate([high, low], axis=0), other_high, dims, preferred_element_type=f32)
        return both[:count] + both[count:] + lax.dot_general(high, other_low, dims, preferred_element_type=f32)

    osc[...] = product(zh, zl, thi, tlo, nn)

    lane = lax.broadcasted_iota(jnp.int32, (LON, 128), 1)
    packed = [jnp.zeros((LON, 128), f32) for _ in range(LAT)]
    for r in range(ROWS):
        value = osc[pl.ds(r, LON, stride=16), :]
        mine = jnp.logical_and(lane >= 10 * r, lane < 10 * r + 10)
        for g in range(LAT):
            shift = (10 * (r - g)) % 128
            moved = pltpu.roll(value, shift, axis=1) if shift else value
            packed[g] = jnp.where(mine, moved, packed[g])
    for g in range(LAT):
        send_b[g * LON : (g + 1) * LON, 0, :] = packed[g]

    def exchange_all(send, recv, which, source, target):
        for a, b in everyone:
            pltpu.make_async_remote_copy(
                send.at[source(a, b)], recv.at[target], ssem.at[which], rsem.at[which], device_id={"lat": a, "lon": b}
            ).start()
        recv[target] = send[source(lat, lon)]

    exchange_all(send_b, recv_b, 1, lambda a, b: a * LON + b, place(lat, lon))

    loads[5].wait()
    loads[6].wait()
    turned = pltpu.roll(resp_ref[...], lax.rem(DEV - me, DEV), axis=1)
    within = lax.broadcasted_iota(jnp.int32, (SLOTS, 128), 1) < DEV - me
    shifted = jnp.where(within, turned[0:SLOTS], turned[1 : SLOTS + 1])
    response = jnp.concatenate(
        [shifted[q : q + 1] for i in range(SLOTS) for q in range(i, SLOTS)], axis=1
    )
    first = jnp.where(jnp.logical_and(lax.broadcasted_iota(jnp.int32, (1, TALL), 1) < MODES, me == 0), 1.0, 2.0)
    response = response * first
    row = lax.broadcasted_iota(jnp.int32, (32, TALL), 0)
    column = lax.broadcasted_iota(jnp.int32, (32, TALL), 1)
    slot = jnp.zeros((32, TALL), jnp.int32)
    for i in range(1, SLOTS):
        slot = slot + jnp.where(column >= STARTS[i], 1, 0)
    wanted = 2 * slot + 16 * (column & 1)
    keep = jnp.logical_or(row == wanted, row == wanted + 1)
    gain = jnp.where(keep, response, 0.0)

    finish(send_b, recv_b, 1, DEV - 1)

    north = recv_b[0:HALF, 0, :]
    southern = recv_b[HALF:DEV, 0, :]
    weights = wt_ref[...]
    folded = jnp.concatenate([(north + southern) * weights, (north - southern) * weights], axis=0)
    fold[...] = folded.T
    left = lax.broadcasted_iota(jnp.int32, (10, 128), 1) < HALF
    evens = []
    odds = []
    for j in range(5):
        first_row = fold[20 * j : 20 * j + 10, :]
        if j < 4:
            second_row = fold[20 * j + 10 : 20 * j + 20, :]
        else:
            second_row = jnp.zeros((10, 128), f32)
        evens.append(jnp.where(left, first_row, pltpu.roll(second_row, HALF, axis=1)))
        odds.append(jnp.where(left, pltpu.roll(first_row, HALF, axis=1), second_row))
    pad = jnp.zeros((6, WIDE), f32)
    lhs = jnp.concatenate([jnp.concatenate(evens, axis=1), pad, jnp.concatenate(odds, axis=1), pad], axis=0)
    lh, ll = split(lhs)
    sh, sl = split(product(lh, ll, phi[...], plo[...], nt) * gain)
    synthesis = product(sh, sl, phi[...], plo[...], nn)
    fold[...] = jnp.zeros((128, 128), f32)
    for j in range(5):
        e = synthesis[0:10, j * 128 : (j + 1) * 128]
        o = synthesis[16:26, j * 128 : (j + 1) * 128]
        n, s = e + o, e - o
        fold[20 * j : 20 * j + 10, :] = jnp.where(left, n, pltpu.roll(s, HALF, axis=1))
        if j < 4:
            fold[20 * j + 10 : 20 * j + 20, :] = jnp.where(left, pltpu.roll(n, HALF, axis=1), s)
    send_c[:, 0, :] = fold[...].T

    exchange_all(send_c, recv_c, 2, place, me)
    finish(send_c, recv_c, 2, DEV - 1)

    pieces = [recv_c[g * LON : (g + 1) * LON, 0, :] for g in range(LAT)]
    gathered = []
    for r in range(ROWS):
        value = jnp.zeros((LON, 128), f32)
        for g in range(LAT):
            mine = jnp.logical_and(lane >= 10 * g, lane < 10 * g + 10)
            shift = (10 * (g - r)) % 128
            moved = pltpu.roll(pieces[g], shift, axis=1) if shift else pieces[g]
            value = jnp.where(mine, moved, value)
        gathered.append(value)
    gh, gl = split(jnp.concatenate(gathered, axis=0))
    inverse = product(gh, gl, thi, tlo, nt)
    for c in range(4):
        vs[c] = inverse[:, c * 128 : (c + 1) * 128]

    for side in range(2):
        lanes = slice(side * 128, side * 128 + 128)
        real = []
        imag = []
        for rho in range(LON):
            tc = tw_ref[0, rho : rho + 1, lanes]
            ts = tw_ref[1, rho : rho + 1, lanes]
            vre = vs[side, pl.ds(rho, ROWS, stride=16), :]
            vim = vs[2 + side, pl.ds(rho, ROWS, stride=16), :]
            real.append(vre * tc - vim * ts)
            imag.append(None if rho % 8 == 0 else vre * ts + vim * tc)
        mine = slice(side * ROWS, side * ROWS + ROWS)
        ure = {rho: real[rho] + real[16 - rho] for rho in range(1, 8)}
        uim = {rho: imag[rho] - imag[16 - rho] for rho in range(1, 8)}
        for b in range(5):
            ge = combine(
                [(real[0], 1.0), (real[8], 1.0 - 2.0 * (b % 2))] + [(ure[q], cosine(q * b)) for q in (2, 4, 6)]
            )
            go = combine([(ure[q], cosine(q * b)) for q in (1, 3, 5, 7)])
            he = combine([(uim[q], sine(q * b)) for q in (2, 4, 6)])
            ho = combine([(uim[q], sine(q * b)) for q in (1, 3, 5, 7)])
            send_d[b, mine, 0, :] = (ge + go) - (he + ho)
            if b > 0:
                send_d[16 - b, mine, 0, :] = (ge + go) + (he + ho)
            if b < 4:
                send_d[8 - b, mine, 0, :] = (ge - go) - (ho - he)
                if b > 0:
                    send_d[8 + b, mine, 0, :] = (ge - go) + (ho - he)

    exchange_lon(send_d, recv_d, 3)
    finish(send_d, recv_d, 3, LON - 1)

    def unstage(block, carry):
        for r in range(ROWS):
            target = jnp.where(south == 1, ROWS - 1 - r, r)
            line = jnp.concatenate([recv_d[block, r], recv_d[block, ROWS + r]], axis=1)
            o_ref[pl.ds(ROWS * block + target, 1), :] = line
        return carry

    lax.fori_loop(0, LON, unstage, 0)


def shards(height, response):
    high, low, twiddle, geometry, weights, first = constants()
    vmem = pl.BlockSpec(memory_space=pltpu.VMEM)
    smem = pl.BlockSpec(memory_space=pltpu.SMEM)
    hbm = pl.BlockSpec(memory_space=pltpu.HBM)
    blocks = pltpu.VMEM((LON, 2 * ROWS, 1, 128), f32)
    rows = pltpu.VMEM((DEV, 1, 128), f32)
    out = pl.pallas_call(
        kernel,
        out_shape=jax.ShapeDtypeStruct((NLAT // LAT, CELLS), f32),
        in_specs=[hbm] * 7 + [smem],
        out_specs=vmem,
        scratch_shapes=[
            pltpu.VMEM((NLAT // LAT, CELLS), f32),
            pltpu.VMEM((8, 128), f32),
            pltpu.VMEM((2 * CELLS, 128), bf16),
            pltpu.VMEM((2 * CELLS, 128), bf16),
            pltpu.VMEM((2, LON, CELLS), f32),
            pltpu.VMEM((4, 8, 128), f32),
            pltpu.VMEM((HALF, 128), f32),
            blocks,
            blocks,
            pltpu.VMEM((LON, 16, 2 * CELLS), f32),
            pltpu.VMEM((LON * 16, 128), f32),
            rows,
            rows,
            pltpu.VMEM((TALL, 128), f32),
            pltpu.VMEM((TALL, 128), f32),
            pltpu.VMEM((TALL * 8, 128), f32),
            pltpu.VMEM((TALL, WIDE), bf16),
            pltpu.VMEM((TALL, WIDE), bf16),
            pltpu.VMEM((128, 128), f32),
            rows,
            rows,
            pltpu.VMEM((4, ROWS * LON, 128), f32),
            blocks,
            blocks,
            pltpu.SemaphoreType.DMA((4,)),
            pltpu.SemaphoreType.DMA((4,)),
            pltpu.SemaphoreType.DMA((7,)),
        ],
        compiler_params=pltpu.CompilerParams(
            collective_id=0, has_side_effects=True, vmem_limit_bytes=60 * 1024 * 1024
        ),
    )(
        height.reshape(NLAT // LAT, CELLS),
        response.reshape(SLOTS, 128),
        jnp.asarray(high),
        jnp.asarray(low),
        jnp.asarray(twiddle),
        jnp.asarray(geometry),
        jnp.asarray(weights),
        jnp.asarray(first),
    )
    return out.reshape(height.shape)


def solution(mesh):
    placed = (P(None, "lat", "lon"), P())
    return jax.shard_map(
        shards, mesh=mesh, in_specs=placed, out_specs=P(None, "lat", "lon"), check_vma=False
    )
```

```python
import math

import jax
import jax.numpy as jnp
import numpy as np
from jax import lax
from jax.experimental import pallas as pl
from jax.experimental.pallas import tpu as pltpu
from jax.sharding import PartitionSpec as P

NLAT = 1152
NLON = 4096
MODES = 640
LON = 16
LAT = 8
DEV = LON * LAT
ROWS = NLAT // DEV
CELLS = NLON // LON
SLOTS = MODES // DEV
HALF = DEV // 2
STARTS = [sum(MODES - DEV * t for t in range(i)) for i in range(SLOTS)]
TALL = sum(MODES - DEV * t for t in range(SLOTS))
WIDE = 640
HOPS = (0, 1, 2, 1)
FAR = sorted(
    [(dy, dx, dz, dc) for dy in range(4) for dx in range(4) for dz in range(4) for dc in range(2)],
    key=lambda o: (-HOPS[o[0]] - HOPS[o[1]] - HOPS[o[2]], -o[3]),
)[: DEV - 1]
FAR_LON = sorted(
    [(dx, dz, dc) for dx in range(2) for dz in range(4) for dc in range(2)],
    key=lambda o: (-o[0] - HOPS[o[1]], -o[2]),
)[: LON - 1]
bf16 = jnp.bfloat16
f32 = jnp.float32


def constants():
    t = np.arange(CELLS)
    table = np.zeros((2 * CELLS, 128))
    for g in range(LAT):
        for i in range(SLOTS):
            angle = 2 * np.pi * ((g + LAT * i) * t % CELLS) / CELLS
            column = (g * SLOTS + i) * 2
            table[:CELLS, column] = np.cos(angle)
            table[CELLS:, column] = np.sin(angle)
            table[:CELLS, column + 1] = -np.sin(angle)
            table[CELLS:, column + 1] = np.cos(angle)
    high = table.astype(np.float32).astype(bf16)
    low = (table - high.astype(np.float64)).astype(np.float32).astype(bf16)
    angle = 2 * np.pi * np.arange(LON)[:, None] * t[None, :] / NLON
    twiddle = np.stack([np.cos(angle), np.sin(angle)]).astype(np.float32)
    geometry = np.zeros((4, 8, 128), np.float32)
    for chunk in range(5):
        for lane in range(128):
            r = 2 * chunk + lane // HALF
            if r < ROWS:
                theta = np.pi * (ROWS * (lane % HALF) + r + 0.5) / NLAT
                log_sine = np.log2(np.sin(theta))
                coarse = np.round(log_sine * 1024) / 1024
                geometry[:, chunk, lane] = np.cos(theta), coarse, log_sine - coarse, 1.0
    weights = np.zeros((HALF, 128), np.float32)
    for r in range(ROWS):
        theta = np.pi * (ROWS * np.arange(HALF) + r + 0.5) / NLAT
        cell = np.sin(theta) * (np.pi / NLAT) * (2 * np.pi / NLON)
        weights[:, 10 * r : 10 * r + 10] = cell[:, None]
    first = [
        (0.5 * (math.lgamma(m + 1.5) - math.lgamma(1.5) - math.lgamma(m + 1.0)) - 0.5 * math.log(4 * math.pi))
        / math.log(2)
        for m in range(MODES)
    ]
    return high, low, twiddle, geometry, weights, np.asarray(first, np.float32)


def split(x):
    high = x.astype(bf16)
    return high, (x - high.astype(f32)).astype(bf16)


def cosine(n):
    return math.cos(math.pi * (n % 16) / 8)


def sine(n):
    return math.sin(math.pi * (n % 16) / 8)


def combine(terms):
    total = None
    for value, factor in terms:
        if abs(factor) < 1e-9:
            continue
        if abs(factor - 1) < 1e-9:
            term, negative = value, False
        elif abs(factor + 1) < 1e-9:
            term, negative = value, True
        else:
            term, negative = value * factor, False
        if total is None:
            total = -term if negative else term
        else:
            total = total - term if negative else total + term
    return 0.0 if total is None else total


def kernel(
    h_hbm, resp_hbm, thi_hbm, tlo_hbm, tw_hbm, geo_hbm, wt_hbm, lc_ref, o_hbm,
    h_ref, resp_ref, thi_ref, tlo_ref, tw_ref, geo_ref, wt_ref,
    send_a, recv_a, zs, osc, send_b, recv_b, coef_a, coef_c, tall, phi, plo, phi_t, plo_t, fold, send_c, recv_c, vs, send_d, recv_d,
    out_ref, ssem, rsem, lsem,
):
    loads = [
        pltpu.make_async_copy(source, target, lsem.at[n])
        for n, (source, target) in enumerate(
            [
                (h_hbm, h_ref),
                (geo_hbm, geo_ref),
                (tw_hbm, tw_ref),
                (thi_hbm, thi_ref),
                (tlo_hbm, tlo_ref),
                (wt_hbm, wt_ref),
                (resp_hbm, resp_ref.at[pl.ds(0, SLOTS)]),
            ]
        )
    ]
    resp_ref[...] = jnp.zeros((8, 128), f32)
    for load in loads:
        load.start()
    lon = lax.axis_index("lon")
    lat = lax.axis_index("lat")
    me = lat * LON + lon
    south = lat // (LAT // 2)
    barrier = pltpu.get_barrier_semaphore()

    y, z, core = lat // 2, (lon // 2) % 4, lon % 2
    x_low = lon // 8
    x_all = (lat % 2) * 2 + x_low
    at_y = [((y + d) % 4) * 2 for d in range(4)]
    at_x = [(x_all + d) % 4 for d in range(4)]
    at_x = [(v // 2, (v % 2) * 8) for v in at_x]
    at_low = [((x_low + d) % 2) * 8 for d in range(2)]
    at_z = [((z + d) % 4) * 2 for d in range(4)]
    at_core = [core, 1 - core]
    everyone = [(at_y[dy] + at_x[dx][0], at_x[dx][1] + at_z[dz] + at_core[dc]) for dy, dx, dz, dc in FAR]
    row_peers = [at_low[dx] + at_z[dz] + at_core[dc] for dx, dz, dc in FAR_LON]

    def place(a, b):
        p = a * LON + b
        return jnp.where(a < LAT // 2, p, DEV + HALF - 1 - p)

    greeted = [(lat, b) for b in row_peers]
    x_high = lat % 2
    same, mirror = lon, (1 - x_low) * 8 + z * 2 + core
    greeted += [(at_y[d] + 1 - x_high, mirror) for d in (2, 1, 3, 0)] + [(at_y[d] + x_high, same) for d in (2, 1, 3)]
    for a, b in greeted:
        pl.semaphore_signal(barrier, inc=1, device_id={"lat": a, "lon": b})

    loads[0].wait()

    def stage(block, carry):
        for r in range(ROWS):
            source = jnp.where(south == 1, ROWS - 1 - r, r)
            line = h_ref[pl.ds(ROWS * block + source, 1), :]
            send_a[0, block, r] = line[:, :128]
            send_a[1, block, r] = line[:, 128:]
        return carry

    lax.fori_loop(0, LON, stage, 0)

    for i in range(SLOTS):
        def coefficients(block, carry, i=i):
            row = block * 32
            m = (DEV * i + me).astype(f32)
            k = (row + lax.broadcasted_iota(jnp.int32, (32, 128), 0)).astype(f32)
            k1 = k + 1.0
            l2 = 2.0 * (m + k1)
            squared = (l2 * l2 - 1.0) / (k1 * (2.0 * m + k1))
            below = l2 - 2.0
            ratio = k * (2.0 * m + k) / jnp.maximum(below * below - 1.0, 1.0)
            start = pl.multiple_of(STARTS[i] + row, 8)
            coef_a[pl.ds(start, 32), :] = jnp.sqrt(squared)
            coef_c[pl.ds(start, 32), :] = jnp.sqrt(squared * ratio)
            return carry

        lax.fori_loop(0, (MODES - DEV * i) // 32, coefficients, 0)

    pl.semaphore_wait(barrier, len(greeted))

    def exchange_lon(send, recv, which):
        for b in row_peers:
            pltpu.make_async_remote_copy(
                send.at[b], recv.at[lon], ssem.at[which], rsem.at[which], device_id={"lat": lat, "lon": b}
            ).start()
        recv[lon] = send[lon]

    def finish(send, recv, which, count):
        every = pltpu.make_async_remote_copy(
            send.at[pl.ds(0, count)], recv.at[pl.ds(0, count)], ssem.at[which], rsem.at[which],
            device_id={"lat": lat, "lon": row_peers[0]},
        )
        every.wait_send()
        every.wait_recv()

    for side in range(2):
        exchange_lon(send_a.at[side], recv_a.at[side], side)

    loads[1].wait()
    x = geo_ref[0]
    state = []
    for i in range(SLOTS):
        m = (DEV * i + me).astype(f32)
        coarse = m * geo_ref[1]
        fine = m * geo_ref[2] + lc_ref[DEV * i + me]
        count = jnp.maximum(jnp.ceil((-84.0 - (coarse + fine)) * (1.0 / 64.0)), 0.0)
        value = jnp.exp2((coarse + 64.0 * count) + fine) * geo_ref[3]
        state.append((jnp.zeros_like(value), value, count))

    for section in range(SLOTS):
        active = SLOTS - section

        def steps(block, carry, section=section, active=active):
            new = []
            for i in range(active):
                earlier, latest, count = carry[i]
                base = STARTS[i] + section * DEV
                row = pl.multiple_of(base + block * 8, 8)
                a8 = coef_a[pl.ds(row, 8), :]
                c8 = coef_c[pl.ds(row, 8), :]
                seen = jnp.where(count == 0.0, 1.0, 0.0)
                for u in range(8):
                    tall[pl.ds(pl.multiple_of((row + u) * 8, 8), 8), :] = latest * seen
                    following = (a8[u : u + 1, :] * x) * latest - c8[u : u + 1, :] * earlier
                    earlier, latest = latest, following
                large = jnp.logical_and(jnp.abs(latest) > 2.0**-20, count > 0.0)
                factor = jnp.where(large, 2.0**-64, 1.0)
                new.append((earlier * factor, latest * factor, count - jnp.where(large, 1.0, 0.0)))
            return tuple(new)

        state = list(lax.fori_loop(0, DEV // 8, steps, tuple(state[:active])))

    def halves(block, carry):
        row = pl.multiple_of(block * 128, 128)
        for j in range(5):
            value = tall[pl.ds(row * 8 + j, 128, stride=8), :]
            high, low = split(value)
            phi[pl.ds(row, 128), j * 128 : (j + 1) * 128] = high
            plo[pl.ds(row, 128), j * 128 : (j + 1) * 128] = low
            high, low = high.T, low.T
            phi_t[j * 128 : (j + 1) * 128, pl.ds(row, 128)] = high
            plo_t[j * 128 : (j + 1) * 128, pl.ds(row, 128)] = low
        return carry

    lax.fori_loop(0, TALL // 128, halves, 0)

    loads[2].wait()
    for side in range(2):
        lanes = slice(side * 128, side * 128 + 128)
        finish(send_a.at[side], recv_a.at[side], side, LON - 1)
        d = [recv_a[side, b, :, 0, :] for b in range(LON)]
        even = {b: d[b] + d[16 - b] for b in range(1, 8)}
        odd = {b: d[b] - d[16 - b] for b in range(1, 8)}
        real = [None] * 9
        imag = [None] * 9
        for rho in range(5):
            a = combine(
                [(d[0], 1.0), (d[8], 1.0 - 2.0 * (rho % 2))] + [(even[b], cosine(rho * b)) for b in (2, 4, 6)]
            )
            b_ = combine([(even[b], cosine(rho * b)) for b in (1, 3, 5, 7)])
            e = combine([(odd[b], -sine(rho * b)) for b in (2, 4, 6)])
            c = combine([(odd[b], -sine(rho * b)) for b in (1, 3, 5, 7)])
            real[rho], real[8 - rho] = a + b_, a - b_
            imag[rho], imag[8 - rho] = c + e, c - e
        for rho in range(LON):
            tc = tw_ref[0, rho : rho + 1, lanes]
            ts = tw_ref[1, rho : rho + 1, lanes]
            if rho % 8 == 0:
                zre, zim = real[rho] * tc, -(real[rho] * ts)
            elif rho < 8:
                zre, zim = real[rho] * tc + imag[rho] * ts, imag[rho] * tc - real[rho] * ts
            else:
                yre, yim = real[16 - rho], imag[16 - rho]
                zre, zim = yre * tc - yim * ts, -(yim * tc) - yre * ts
            zs[rho, 0:ROWS, lanes] = zre
            zs[rho, 0:ROWS, CELLS + side * 128 : CELLS + side * 128 + 128] = zim

    loads[3].wait()
    loads[4].wait()
    zh, zl = split(zs[...].reshape(LON * 16, 2 * CELLS))
    thi = thi_ref[...]
    tlo = tlo_ref[...]
    nn = (((1,), (0,)), ((), ()))
    nt = (((1,), (1,)), ((), ()))

    def product(high, low, other_high, other_low, dims):
        count = high.shape[0]
        both = lax.dot_general(jnp.concatenate([high, low], axis=0), other_high, dims, preferred_element_type=f32)
        return both[:count] + both[count:] + lax.dot_general(high, other_low, dims, preferred_element_type=f32)

    osc[...] = product(zh, zl, thi, tlo, nn)

    lane = lax.broadcasted_iota(jnp.int32, (LON, 128), 1)
    packed = [jnp.zeros((LON, 128), f32) for _ in range(LAT)]
    for r in range(ROWS):
        value = osc[pl.ds(r, LON, stride=16), :]
        mine = jnp.logical_and(lane >= 10 * r, lane < 10 * r + 10)
        for g in range(LAT):
            shift = (10 * (r - g)) % 128
            moved = pltpu.roll(value, shift, axis=1) if shift else value
            packed[g] = jnp.where(mine, moved, packed[g])
    for g in range(LAT):
        send_b[g * LON : (g + 1) * LON, 0, :] = packed[g]

    def exchange_all(send, recv, which, source, target):
        for a, b in everyone:
            pltpu.make_async_remote_copy(
                send.at[source(a, b)], recv.at[target], ssem.at[which], rsem.at[which], device_id={"lat": a, "lon": b}
            ).start()
        recv[target] = send[source(lat, lon)]

    exchange_all(send_b, recv_b, 2, lambda a, b: a * LON + b, place(lat, lon))

    loads[5].wait()
    loads[6].wait()
    turned = pltpu.roll(resp_ref[...], lax.rem(DEV - me, DEV), axis=1)
    within = lax.broadcasted_iota(jnp.int32, (SLOTS, 128), 1) < DEV - me
    shifted = jnp.where(within, turned[0:SLOTS], turned[1 : SLOTS + 1])
    response = jnp.concatenate(
        [shifted[q : q + 1] for i in range(SLOTS) for q in range(i, SLOTS)], axis=1
    )
    first = jnp.where(jnp.logical_and(lax.broadcasted_iota(jnp.int32, (1, TALL), 1) < MODES, me == 0), 1.0, 2.0)
    response = response * first
    row = lax.broadcasted_iota(jnp.int32, (32, TALL), 0)
    column = lax.broadcasted_iota(jnp.int32, (32, TALL), 1)
    slot = jnp.zeros((32, TALL), jnp.int32)
    for i in range(1, SLOTS):
        slot = slot + jnp.where(column >= STARTS[i], 1, 0)
    wanted = 2 * slot + 16 * (column & 1)
    keep = jnp.logical_or(row == wanted, row == wanted + 1)
    gain = jnp.where(keep, response, 0.0)

    finish(send_b, recv_b, 2, DEV - 1)

    north = recv_b[0:HALF, 0, :]
    southern = recv_b[HALF:DEV, 0, :]
    weights = wt_ref[...]
    folded = jnp.concatenate([(north + southern) * weights, (north - southern) * weights], axis=0)
    fold[...] = folded.T
    left = lax.broadcasted_iota(jnp.int32, (10, 128), 1) < HALF
    evens = []
    odds = []
    for j in range(5):
        first_row = fold[20 * j : 20 * j + 10, :]
        if j < 4:
            second_row = fold[20 * j + 10 : 20 * j + 20, :]
        else:
            second_row = jnp.zeros((10, 128), f32)
        evens.append(jnp.where(left, first_row, pltpu.roll(second_row, HALF, axis=1)))
        odds.append(jnp.where(left, pltpu.roll(first_row, HALF, axis=1), second_row))
    pad = jnp.zeros((6, WIDE), f32)
    lhs = jnp.concatenate([jnp.concatenate(evens, axis=1), pad, jnp.concatenate(odds, axis=1), pad], axis=0)
    lh, ll = split(lhs)
    sh, sl = split(product(lh, ll, phi_t[...], plo_t[...], nn) * gain)
    synthesis = product(sh, sl, phi[...], plo[...], nn)
    fold[...] = jnp.zeros((128, 128), f32)
    for j in range(5):
        e = synthesis[0:10, j * 128 : (j + 1) * 128]
        o = synthesis[16:26, j * 128 : (j + 1) * 128]
        n, s = e + o, e - o
        fold[20 * j : 20 * j + 10, :] = jnp.where(left, n, pltpu.roll(s, HALF, axis=1))
        if j < 4:
            fold[20 * j + 10 : 20 * j + 20, :] = jnp.where(left, pltpu.roll(n, HALF, axis=1), s)
    send_c[:, 0, :] = fold[...].T

    exchange_all(send_c, recv_c, 3, place, me)
    finish(send_c, recv_c, 3, DEV - 1)

    pieces = [recv_c[g * LON : (g + 1) * LON, 0, :] for g in range(LAT)]
    gathered = []
    for r in range(ROWS):
        value = jnp.zeros((LON, 128), f32)
        for g in range(LAT):
            mine = jnp.logical_and(lane >= 10 * g, lane < 10 * g + 10)
            shift = (10 * (g - r)) % 128
            moved = pltpu.roll(pieces[g], shift, axis=1) if shift else pieces[g]
            value = jnp.where(mine, moved, value)
        gathered.append(value)
    gh, gl = split(jnp.concatenate(gathered, axis=0))
    inverse = product(gh, gl, thi, tlo, nt)
    for c in range(4):
        vs[c] = inverse[:, c * 128 : (c + 1) * 128]

    for side in range(2):
        lanes = slice(side * 128, side * 128 + 128)
        real = []
        imag = []
        for rho in range(LON):
            tc = tw_ref[0, rho : rho + 1, lanes]
            ts = tw_ref[1, rho : rho + 1, lanes]
            vre = vs[side, pl.ds(rho, ROWS, stride=16), :]
            vim = vs[2 + side, pl.ds(rho, ROWS, stride=16), :]
            real.append(vre * tc - vim * ts)
            imag.append(None if rho % 8 == 0 else vre * ts + vim * tc)
        ure = {rho: real[rho] + real[16 - rho] for rho in range(1, 8)}
        uim = {rho: imag[rho] - imag[16 - rho] for rho in range(1, 8)}
        def put(b, value, side=side):
            for r in range(ROWS):
                send_d[side, b, jnp.where(south == 1, ROWS - 1 - r, r)] = value[r : r + 1]

        for b in range(5):
            ge = combine(
                [(real[0], 1.0), (real[8], 1.0 - 2.0 * (b % 2))] + [(ure[q], cosine(q * b)) for q in (2, 4, 6)]
            )
            go = combine([(ure[q], cosine(q * b)) for q in (1, 3, 5, 7)])
            he = combine([(uim[q], sine(q * b)) for q in (2, 4, 6)])
            ho = combine([(uim[q], sine(q * b)) for q in (1, 3, 5, 7)])
            put(b, (ge + go) - (he + ho))
            if b > 0:
                put(16 - b, (ge + go) + (he + ho))
            if b < 4:
                put(8 - b, (ge - go) - (ho - he))
                if b > 0:
                    put(8 + b, (ge - go) + (ho - he))
        exchange_lon(send_d.at[side], recv_d.at[side], 4 + side)

    stores = []
    for side in range(2):
        lanes = slice(side * 128, side * 128 + 128)
        finish(send_d.at[side], recv_d.at[side], 4 + side, LON - 1)
        for b in range(LON):
            out_ref[ROWS * b : ROWS * b + ROWS, lanes] = recv_d[side, b, :, 0, :]
        store = pltpu.make_async_copy(out_ref.at[:, lanes], o_hbm.at[:, lanes], lsem.at[7 + side])
        store.start()
        stores.append(store)
    for store in stores:
        store.wait()


def shards(height, response):
    high, low, twiddle, geometry, weights, first = constants()
    smem = pl.BlockSpec(memory_space=pltpu.SMEM)
    hbm = pl.BlockSpec(memory_space=pltpu.HBM)
    blocks = pltpu.VMEM((2, LON, ROWS, 1, 128), f32)
    rows = pltpu.VMEM((DEV, 1, 128), f32)
    out = pl.pallas_call(
        kernel,
        out_shape=jax.ShapeDtypeStruct((NLAT // LAT, CELLS), f32),
        in_specs=[hbm] * 7 + [smem],
        out_specs=hbm,
        scratch_shapes=[
            pltpu.VMEM((NLAT // LAT, CELLS), f32),
            pltpu.VMEM((8, 128), f32),
            pltpu.VMEM((2 * CELLS, 128), bf16),
            pltpu.VMEM((2 * CELLS, 128), bf16),
            pltpu.VMEM((2, LON, CELLS), f32),
            pltpu.VMEM((4, 8, 128), f32),
            pltpu.VMEM((HALF, 128), f32),
            blocks,
            blocks,
            pltpu.VMEM((LON, 16, 2 * CELLS), f32),
            pltpu.VMEM((LON * 16, 128), f32),
            rows,
            rows,
            pltpu.VMEM((TALL, 128), f32),
            pltpu.VMEM((TALL, 128), f32),
            pltpu.VMEM((TALL * 8, 128), f32),
            pltpu.VMEM((TALL, WIDE), bf16),
            pltpu.VMEM((TALL, WIDE), bf16),
            pltpu.VMEM((WIDE, TALL), bf16),
            pltpu.VMEM((WIDE, TALL), bf16),
            pltpu.VMEM((128, 128), f32),
            rows,
            rows,
            pltpu.VMEM((4, ROWS * LON, 128), f32),
            blocks,
            blocks,
            pltpu.VMEM((NLAT // LAT, CELLS), f32),
            pltpu.SemaphoreType.DMA((6,)),
            pltpu.SemaphoreType.DMA((6,)),
            pltpu.SemaphoreType.DMA((9,)),
        ],
        compiler_params=pltpu.CompilerParams(
            collective_id=0, has_side_effects=True, vmem_limit_bytes=60 * 1024 * 1024
        ),
    )(
        height.reshape(NLAT // LAT, CELLS),
        response.reshape(SLOTS, 128),
        jnp.asarray(high),
        jnp.asarray(low),
        jnp.asarray(twiddle),
        jnp.asarray(geometry),
        jnp.asarray(weights),
        jnp.asarray(first),
    )
    return out.reshape(height.shape)


def solution(mesh):
    placed = (P(None, "lat", "lon"), P())
    return jax.shard_map(
        shards, mesh=mesh, in_specs=placed, out_specs=P(None, "lat", "lon"), check_vma=False
    )
```

```python
import math

import jax
import jax.numpy as jnp
import numpy as np
from jax import lax
from jax.experimental import pallas as pl
from jax.experimental.pallas import tpu as pltpu
from jax.sharding import PartitionSpec as P

NLAT = 1152
NLON = 4096
MODES = 640
LON = 16
LAT = 8
DEV = LON * LAT
ROWS = NLAT // DEV
CELLS = NLON // LON
SLOTS = MODES // DEV
HALF = DEV // 2
STARTS = [sum(MODES - DEV * t for t in range(i)) for i in range(SLOTS)]
TALL = sum(MODES - DEV * t for t in range(SLOTS))
WIDE = 640
HOPS = (0, 1, 2, 1)
FAR = sorted(
    [(dy, dx, dz, dc) for dy in range(4) for dx in range(4) for dz in range(4) for dc in range(2)],
    key=lambda o: (-HOPS[o[0]] - HOPS[o[1]] - HOPS[o[2]], -o[3]),
)[: DEV - 1]
FAR_LON = sorted(
    [(dx, dz, dc) for dx in range(2) for dz in range(4) for dc in range(2)],
    key=lambda o: (-o[0] - HOPS[o[1]], -o[2]),
)[: LON - 1]
bf16 = jnp.bfloat16
f32 = jnp.float32


def constants():
    t = np.arange(CELLS)
    table = np.zeros((2 * CELLS, 128))
    for g in range(LAT):
        for i in range(SLOTS):
            angle = 2 * np.pi * ((g + LAT * i) * t % CELLS) / CELLS
            column = (g * SLOTS + i) * 2
            table[:CELLS, column] = np.cos(angle)
            table[CELLS:, column] = np.sin(angle)
            table[:CELLS, column + 1] = -np.sin(angle)
            table[CELLS:, column + 1] = np.cos(angle)
    high = table.astype(np.float32).astype(bf16)
    low = (table - high.astype(np.float64)).astype(np.float32).astype(bf16)
    angle = 2 * np.pi * np.arange(LON)[:, None] * t[None, :] / NLON
    twiddle = np.stack([np.cos(angle), np.sin(angle)]).astype(np.float32)
    geometry = np.zeros((5, 8, 128), np.float32)
    for chunk in range(5):
        for lane in range(128):
            r = 2 * chunk + lane // HALF
            if r < ROWS:
                theta = np.pi * (ROWS * (lane % HALF) + r + 0.5) / NLAT
                log_sine = np.log2(np.sin(theta))
                coarse = np.round(log_sine * 1024) / 1024
                geometry[:4, chunk, lane] = np.cos(theta), coarse, log_sine - coarse, 1.0
    weights = np.zeros((HALF, 128), np.float32)
    for r in range(ROWS):
        theta = np.pi * (ROWS * np.arange(HALF) + r + 0.5) / NLAT
        cell = np.sin(theta) * (np.pi / NLAT) * (2 * np.pi / NLON)
        weights[:, 10 * r : 10 * r + 10] = cell[:, None]
    first = [
        (0.5 * (math.lgamma(m + 1.5) - math.lgamma(1.5) - math.lgamma(m + 1.0)) - 0.5 * math.log(4 * math.pi))
        / math.log(2)
        for m in range(MODES)
    ]
    geometry[4, :SLOTS] = np.reshape(first, (SLOTS, DEV))
    return high, low, twiddle, geometry, weights


def split(x):
    high = x.astype(bf16)
    return high, (x - high.astype(f32)).astype(bf16)


def cosine(n):
    return math.cos(math.pi * (n % 16) / 8)


def sine(n):
    return math.sin(math.pi * (n % 16) / 8)


def combine(terms):
    total = None
    for value, factor in terms:
        if abs(factor) < 1e-9:
            continue
        if abs(factor - 1) < 1e-9:
            term, negative = value, False
        elif abs(factor + 1) < 1e-9:
            term, negative = value, True
        else:
            term, negative = value * factor, False
        if total is None:
            total = -term if negative else term
        else:
            total = total - term if negative else total + term
    return 0.0 if total is None else total


def kernel(
    h_hbm, resp_hbm, thi_hbm, tlo_hbm, tw_hbm, geo_hbm, wt_hbm, o_hbm,
    h_ref, resp_ref, thi_ref, tlo_ref, tw_ref, geo_ref, wt_ref,
    send_a, recv_a, zs, osc, send_b, recv_b, coef_a, coef_c, tall, phi, plo, phi_t, plo_t, fold, send_c, recv_c, vs, send_d, recv_d,
    ssem, rsem, lsem,
):
    loads = [
        pltpu.make_async_copy(source, target, lsem.at[n])
        for n, (source, target) in enumerate(
            [
                (h_hbm, h_ref),
                (geo_hbm, geo_ref),
                (tw_hbm, tw_ref),
                (thi_hbm, thi_ref),
                (tlo_hbm, tlo_ref),
                (wt_hbm, wt_ref),
                (resp_hbm, resp_ref.at[pl.ds(0, SLOTS)]),
            ]
        )
    ]
    resp_ref[...] = jnp.zeros((8, 128), f32)
    for load in loads:
        load.start()
    lon = lax.axis_index("lon")
    lat = lax.axis_index("lat")
    me = lat * LON + lon
    south = lat // (LAT // 2)
    barrier = pltpu.get_barrier_semaphore()

    y, z, core = lat // 2, (lon // 2) % 4, lon % 2
    x_low = lon // 8
    x_all = (lat % 2) * 2 + x_low
    at_y = [((y + d) % 4) * 2 for d in range(4)]
    at_x = [(x_all + d) % 4 for d in range(4)]
    at_x = [(v // 2, (v % 2) * 8) for v in at_x]
    at_low = [((x_low + d) % 2) * 8 for d in range(2)]
    at_z = [((z + d) % 4) * 2 for d in range(4)]
    at_core = [core, 1 - core]
    everyone = [(at_y[dy] + at_x[dx][0], at_x[dx][1] + at_z[dz] + at_core[dc]) for dy, dx, dz, dc in FAR]
    row_peers = [at_low[dx] + at_z[dz] + at_core[dc] for dx, dz, dc in FAR_LON]

    def place(a, b):
        p = a * LON + b
        return jnp.where(a < LAT // 2, p, DEV + HALF - 1 - p)

    greeted = [(lat, b) for b in row_peers]
    x_high = lat % 2
    same, mirror = lon, (1 - x_low) * 8 + z * 2 + core
    greeted += [(at_y[d] + 1 - x_high, mirror) for d in (2, 1, 3, 0)] + [(at_y[d] + x_high, same) for d in (2, 1, 3)]
    for a, b in greeted:
        pl.semaphore_signal(barrier, inc=1, device_id={"lat": a, "lon": b})

    loads[0].wait()

    def stage(block, carry):
        for r in range(ROWS):
            source = jnp.where(south == 1, ROWS - 1 - r, r)
            line = h_ref[pl.ds(ROWS * block + source, 1), :]
            send_a[0, block, r] = line[:, :128]
            send_a[1, block, r] = line[:, 128:]
        return carry

    lax.fori_loop(0, LON, stage, 0)

    for i in range(SLOTS):
        def coefficients(block, carry, i=i):
            row = block * 32
            m = (DEV * i + me).astype(f32)
            k = (row + lax.broadcasted_iota(jnp.int32, (32, 128), 0)).astype(f32)
            k1 = k + 1.0
            l2 = 2.0 * (m + k1)
            squared = (l2 * l2 - 1.0) / (k1 * (2.0 * m + k1))
            below = l2 - 2.0
            ratio = k * (2.0 * m + k) / jnp.maximum(below * below - 1.0, 1.0)
            start = pl.multiple_of(STARTS[i] + row, 8)
            coef_a[pl.ds(start, 32), :] = jnp.sqrt(squared)
            coef_c[pl.ds(start, 32), :] = jnp.sqrt(squared * ratio)
            return carry

        lax.fori_loop(0, (MODES - DEV * i) // 32, coefficients, 0)

    pl.semaphore_wait(barrier, len(greeted))

    def exchange_lon(send, recv, which):
        for b in row_peers:
            pltpu.make_async_remote_copy(
                send.at[b], recv.at[lon], ssem.at[which], rsem.at[which], device_id={"lat": lat, "lon": b}
            ).start()
        recv[lon] = send[lon]

    def finish(send, recv, which, count):
        every = pltpu.make_async_remote_copy(
            send.at[pl.ds(0, count)], recv.at[pl.ds(0, count)], ssem.at[which], rsem.at[which],
            device_id={"lat": lat, "lon": row_peers[0]},
        )
        every.wait_send()
        every.wait_recv()

    for side in range(2):
        exchange_lon(send_a.at[side], recv_a.at[side], side)

    loads[1].wait()
    x = geo_ref[0]
    starts = pltpu.roll(geo_ref[4], lax.rem(DEV - me, DEV), axis=1)
    state = []
    for i in range(SLOTS):
        m = (DEV * i + me).astype(f32)
        coarse = m * geo_ref[1]
        fine = m * geo_ref[2] + jnp.broadcast_to(starts[i : i + 1, 0:1], (8, 128))
        count = jnp.maximum(jnp.ceil((-84.0 - (coarse + fine)) * (1.0 / 64.0)), 0.0)
        value = jnp.exp2((coarse + 64.0 * count) + fine) * geo_ref[3]
        state.append((jnp.zeros_like(value), value, count))

    for section in range(SLOTS):
        active = SLOTS - section

        def steps(block, carry, section=section, active=active):
            new = []
            for i in range(active):
                earlier, latest, count = carry[i]
                base = STARTS[i] + section * DEV
                row = pl.multiple_of(base + block * 8, 8)
                a8 = coef_a[pl.ds(row, 8), :]
                c8 = coef_c[pl.ds(row, 8), :]
                seen = jnp.where(count == 0.0, 1.0, 0.0)
                for u in range(8):
                    tall[pl.ds(pl.multiple_of((row + u) * 8, 8), 8), :] = latest * seen
                    following = (a8[u : u + 1, :] * x) * latest - c8[u : u + 1, :] * earlier
                    earlier, latest = latest, following
                large = jnp.logical_and(jnp.abs(latest) > 2.0**-20, count > 0.0)
                factor = jnp.where(large, 2.0**-64, 1.0)
                new.append((earlier * factor, latest * factor, count - jnp.where(large, 1.0, 0.0)))
            return tuple(new)

        state = list(lax.fori_loop(0, DEV // 8, steps, tuple(state[:active])))

    loads[2].wait()
    for side in range(2):
        lanes = slice(side * 128, side * 128 + 128)
        finish(send_a.at[side], recv_a.at[side], side, LON - 1)
        d = [recv_a[side, b, :, 0, :] for b in range(LON)]
        even = {b: d[b] + d[16 - b] for b in range(1, 8)}
        odd = {b: d[b] - d[16 - b] for b in range(1, 8)}
        real = [None] * 9
        imag = [None] * 9
        for rho in range(5):
            a = combine(
                [(d[0], 1.0), (d[8], 1.0 - 2.0 * (rho % 2))] + [(even[b], cosine(rho * b)) for b in (2, 4, 6)]
            )
            b_ = combine([(even[b], cosine(rho * b)) for b in (1, 3, 5, 7)])
            e = combine([(odd[b], -sine(rho * b)) for b in (2, 4, 6)])
            c = combine([(odd[b], -sine(rho * b)) for b in (1, 3, 5, 7)])
            real[rho], real[8 - rho] = a + b_, a - b_
            imag[rho], imag[8 - rho] = c + e, c - e
        for rho in range(LON):
            tc = tw_ref[0, rho : rho + 1, lanes]
            ts = tw_ref[1, rho : rho + 1, lanes]
            if rho % 8 == 0:
                zre, zim = real[rho] * tc, -(real[rho] * ts)
            elif rho < 8:
                zre, zim = real[rho] * tc + imag[rho] * ts, imag[rho] * tc - real[rho] * ts
            else:
                yre, yim = real[16 - rho], imag[16 - rho]
                zre, zim = yre * tc - yim * ts, -(yim * tc) - yre * ts
            zs[rho, 0:ROWS, lanes] = zre
            zs[rho, 0:ROWS, CELLS + side * 128 : CELLS + side * 128 + 128] = zim

    loads[3].wait()
    loads[4].wait()
    zh, zl = split(zs[...].reshape(LON * 16, 2 * CELLS))
    thi = thi_ref[...]
    tlo = tlo_ref[...]
    nn = (((1,), (0,)), ((), ()))
    nt = (((1,), (1,)), ((), ()))

    def product(high, low, other_high, other_low, dims):
        count = high.shape[0]
        both = lax.dot_general(jnp.concatenate([high, low], axis=0), other_high, dims, preferred_element_type=f32)
        return both[:count] + both[count:] + lax.dot_general(high, other_low, dims, preferred_element_type=f32)

    osc[...] = product(zh, zl, thi, tlo, nn)

    lane = lax.broadcasted_iota(jnp.int32, (LON, 128), 1)
    packed = [jnp.zeros((LON, 128), f32) for _ in range(LAT)]
    for r in range(ROWS):
        value = osc[pl.ds(r, LON, stride=16), :]
        mine = jnp.logical_and(lane >= 10 * r, lane < 10 * r + 10)
        for g in range(LAT):
            shift = (10 * (r - g)) % 128
            moved = pltpu.roll(value, shift, axis=1) if shift else value
            packed[g] = jnp.where(mine, moved, packed[g])
    for g in range(LAT):
        send_b[g * LON : (g + 1) * LON, :] = packed[g]

    def exchange_all(send, recv, which, source, target):
        for a, b in everyone:
            pltpu.make_async_remote_copy(
                send.at[pl.ds(source(a, b), 1)], recv.at[pl.ds(target, 1)], ssem.at[which], rsem.at[which],
                device_id={"lat": a, "lon": b},
            ).start()
        recv[pl.ds(target, 1), :] = send[pl.ds(source(lat, lon), 1), :]

    exchange_all(send_b, recv_b, 2, lambda a, b: a * LON + b, place(lat, lon))

    def halves(block, carry):
        row = pl.multiple_of(block * 128, 128)
        for j in range(5):
            value = tall[pl.ds(row * 8 + j, 128, stride=8), :]
            high, low = split(value)
            phi[pl.ds(row, 128), j * 128 : (j + 1) * 128] = high
            plo[pl.ds(row, 128), j * 128 : (j + 1) * 128] = low
            high, low = high.T, low.T
            phi_t[j * 128 : (j + 1) * 128, pl.ds(row, 128)] = high
            plo_t[j * 128 : (j + 1) * 128, pl.ds(row, 128)] = low
        return carry

    lax.fori_loop(0, TALL // 128, halves, 0)

    loads[5].wait()
    loads[6].wait()
    turned = pltpu.roll(resp_ref[...], lax.rem(DEV - me, DEV), axis=1)
    within = lax.broadcasted_iota(jnp.int32, (SLOTS, 128), 1) < DEV - me
    shifted = jnp.where(within, turned[0:SLOTS], turned[1 : SLOTS + 1])
    response = jnp.concatenate(
        [shifted[q : q + 1] for i in range(SLOTS) for q in range(i, SLOTS)], axis=1
    )
    first = jnp.where(jnp.logical_and(lax.broadcasted_iota(jnp.int32, (1, TALL), 1) < MODES, me == 0), 1.0, 2.0)
    response = response * first
    row = lax.broadcasted_iota(jnp.int32, (32, TALL), 0)
    column = lax.broadcasted_iota(jnp.int32, (32, TALL), 1)
    slot = jnp.zeros((32, TALL), jnp.int32)
    for i in range(1, SLOTS):
        slot = slot + jnp.where(column >= STARTS[i], 1, 0)
    wanted = 2 * slot + 16 * (column & 1)
    keep = jnp.logical_or(row == wanted, row == wanted + 1)
    gain = jnp.where(keep, response, 0.0)

    finish(send_b, recv_b, 2, DEV - 1)

    north = recv_b[0:HALF, :]
    southern = recv_b[HALF:DEV, :]
    weights = wt_ref[...]
    folded = jnp.concatenate([(north + southern) * weights, (north - southern) * weights], axis=0)
    fold[...] = folded.T
    left = lax.broadcasted_iota(jnp.int32, (10, 128), 1) < HALF
    evens = []
    odds = []
    for j in range(5):
        first_row = fold[20 * j : 20 * j + 10, :]
        if j < 4:
            second_row = fold[20 * j + 10 : 20 * j + 20, :]
        else:
            second_row = jnp.zeros((10, 128), f32)
        evens.append(jnp.where(left, first_row, pltpu.roll(second_row, HALF, axis=1)))
        odds.append(jnp.where(left, pltpu.roll(first_row, HALF, axis=1), second_row))
    pad = jnp.zeros((6, WIDE), f32)
    lhs = jnp.concatenate([jnp.concatenate(evens, axis=1), pad, jnp.concatenate(odds, axis=1), pad], axis=0)
    lh, ll = split(lhs)
    sh, sl = split(product(lh, ll, phi_t[...], plo_t[...], nn) * gain)
    synthesis = product(sh, sl, phi[...], plo[...], nn)
    fold[...] = jnp.zeros((128, 128), f32)
    for j in range(5):
        e = synthesis[0:10, j * 128 : (j + 1) * 128]
        o = synthesis[16:26, j * 128 : (j + 1) * 128]
        n, s = e + o, e - o
        fold[20 * j : 20 * j + 10, :] = jnp.where(left, n, pltpu.roll(s, HALF, axis=1))
        if j < 4:
            fold[20 * j + 10 : 20 * j + 20, :] = jnp.where(left, pltpu.roll(n, HALF, axis=1), s)
    send_c[...] = fold[...].T

    exchange_all(send_c, recv_c, 3, place, me)
    finish(send_c, recv_c, 3, DEV - 1)

    pieces = [recv_c[g * LON : (g + 1) * LON, :] for g in range(LAT)]
    gathered = []
    for r in range(ROWS):
        value = jnp.zeros((LON, 128), f32)
        for g in range(LAT):
            mine = jnp.logical_and(lane >= 10 * g, lane < 10 * g + 10)
            shift = (10 * (g - r)) % 128
            moved = pltpu.roll(pieces[g], shift, axis=1) if shift else pieces[g]
            value = jnp.where(mine, moved, value)
        gathered.append(value)
    gh, gl = split(jnp.concatenate(gathered, axis=0))
    inverse = product(gh, gl, thi, tlo, nt)
    for c in range(4):
        vs[c] = inverse[:, c * 128 : (c + 1) * 128]

    for side in range(2):
        lanes = slice(side * 128, side * 128 + 128)
        real = []
        imag = []
        for rho in range(LON):
            tc = tw_ref[0, rho : rho + 1, lanes]
            ts = tw_ref[1, rho : rho + 1, lanes]
            vre = vs[side, pl.ds(rho, ROWS, stride=16), :]
            vim = vs[2 + side, pl.ds(rho, ROWS, stride=16), :]
            real.append(vre * tc - vim * ts)
            imag.append(None if rho % 8 == 0 else vre * ts + vim * tc)
        ure = {rho: real[rho] + real[16 - rho] for rho in range(1, 8)}
        uim = {rho: imag[rho] - imag[16 - rho] for rho in range(1, 8)}
        def put(b, value, side=side):
            for r in range(ROWS):
                target = ROWS * b + jnp.where(south == 1, ROWS - 1 - r, r)
                send_d[side, pl.ds(target, 1), :] = value[r : r + 1]

        for b in range(5):
            ge = combine(
                [(real[0], 1.0), (real[8], 1.0 - 2.0 * (b % 2))] + [(ure[q], cosine(q * b)) for q in (2, 4, 6)]
            )
            go = combine([(ure[q], cosine(q * b)) for q in (1, 3, 5, 7)])
            he = combine([(uim[q], sine(q * b)) for q in (2, 4, 6)])
            ho = combine([(uim[q], sine(q * b)) for q in (1, 3, 5, 7)])
            put(b, (ge + go) - (he + ho))
            if b > 0:
                put(16 - b, (ge + go) + (he + ho))
            if b < 4:
                put(8 - b, (ge - go) - (ho - he))
                if b > 0:
                    put(8 + b, (ge - go) + (ho - he))
        for b in row_peers:
            pltpu.make_async_remote_copy(
                send_d.at[side, pl.ds(ROWS * b, ROWS)], recv_d.at[side, pl.ds(ROWS * lon, ROWS)],
                ssem.at[4 + side], rsem.at[4 + side], device_id={"lat": lat, "lon": b},
            ).start()
        for r in range(ROWS):
            recv_d[side, pl.ds(ROWS * lon + r, 1), :] = send_d[side, pl.ds(ROWS * lon + r, 1), :]

    stores = []
    for side in range(2):
        lanes = slice(side * 128, side * 128 + 128)
        finish(send_d.at[side], recv_d.at[side], 4 + side, ROWS * (LON - 1))
        store = pltpu.make_async_copy(recv_d.at[side], o_hbm.at[:, lanes], lsem.at[7 + side])
        store.start()
        stores.append(store)
    for store in stores:
        store.wait()


def shards(height, response):
    high, low, twiddle, geometry, weights = constants()
    hbm = pl.BlockSpec(memory_space=pltpu.HBM)
    blocks = pltpu.VMEM((2, LON, ROWS, 1, 128), f32)
    rows = pltpu.VMEM((DEV, 128), f32)
    out = pl.pallas_call(
        kernel,
        out_shape=jax.ShapeDtypeStruct((NLAT // LAT, CELLS), f32),
        in_specs=[hbm] * 7,
        out_specs=hbm,
        scratch_shapes=[
            pltpu.VMEM((NLAT // LAT, CELLS), f32),
            pltpu.VMEM((8, 128), f32),
            pltpu.VMEM((2 * CELLS, 128), bf16),
            pltpu.VMEM((2 * CELLS, 128), bf16),
            pltpu.VMEM((2, LON, CELLS), f32),
            pltpu.VMEM((5, 8, 128), f32),
            pltpu.VMEM((HALF, 128), f32),
            blocks,
            blocks,
            pltpu.VMEM((LON, 16, 2 * CELLS), f32),
            pltpu.VMEM((LON * 16, 128), f32),
            rows,
            rows,
            pltpu.VMEM((TALL, 128), f32),
            pltpu.VMEM((TALL, 128), f32),
            pltpu.VMEM((TALL * 8, 128), f32),
            pltpu.VMEM((TALL, WIDE), bf16),
            pltpu.VMEM((TALL, WIDE), bf16),
            pltpu.VMEM((WIDE, TALL), bf16),
            pltpu.VMEM((WIDE, TALL), bf16),
            pltpu.VMEM((128, 128), f32),
            rows,
            rows,
            pltpu.VMEM((4, ROWS * LON, 128), f32),
            pltpu.VMEM((2, NLAT // LAT, 128), f32),
            pltpu.VMEM((2, NLAT // LAT, 128), f32),
            pltpu.SemaphoreType.DMA((6,)),
            pltpu.SemaphoreType.DMA((6,)),
            pltpu.SemaphoreType.DMA((9,)),
        ],
        compiler_params=pltpu.CompilerParams(
            collective_id=0, has_side_effects=True, vmem_limit_bytes=60 * 1024 * 1024
        ),
    )(
        height.reshape(NLAT // LAT, CELLS),
        response.reshape(SLOTS, 128),
        jnp.asarray(high),
        jnp.asarray(low),
        jnp.asarray(twiddle),
        jnp.asarray(geometry),
        jnp.asarray(weights),
    )
    return out.reshape(height.shape)


def solution(mesh):
    placed = (P(None, "lat", "lon"), P())
    return jax.shard_map(
        shards, mesh=mesh, in_specs=placed, out_specs=P(None, "lat", "lon"), check_vma=False
    )
```

```python
import math

import jax
import jax.numpy as jnp
import numpy as np
from jax import lax
from jax.experimental import pallas as pl
from jax.experimental.pallas import tpu as pltpu
from jax.sharding import PartitionSpec as P

NLAT = 1152
NLON = 4096
MODES = 640
LON = 16
LAT = 8
DEV = LON * LAT
ROWS = NLAT // DEV
CELLS = NLON // LON
SLOTS = MODES // DEV
HALF = DEV // 2
STARTS = [sum(MODES - DEV * t for t in range(i)) for i in range(SLOTS)]
TALL = sum(MODES - DEV * t for t in range(SLOTS))
WIDE = 640
HOPS = (0, 1, 2, 1)
FAR = sorted(
    [(dy, dx, dz, dc) for dy in range(4) for dx in range(4) for dz in range(4) for dc in range(2)],
    key=lambda o: (-HOPS[o[0]] - HOPS[o[1]] - HOPS[o[2]], -o[3]),
)[: DEV - 1]
FAR_LON = sorted(
    [(dx, dz, dc) for dx in range(2) for dz in range(4) for dc in range(2)],
    key=lambda o: (-o[0] - HOPS[o[1]], -o[2]),
)[: LON - 1]
bf16 = jnp.bfloat16
f32 = jnp.float32


def constants():
    t = np.arange(CELLS)
    table = np.zeros((2 * CELLS, 128))
    for g in range(LAT):
        for i in range(SLOTS):
            angle = 2 * np.pi * ((g + LAT * i) * t % CELLS) / CELLS
            column = (g * SLOTS + i) * 2
            table[:CELLS, column] = np.cos(angle)
            table[CELLS:, column] = np.sin(angle)
            table[:CELLS, column + 1] = -np.sin(angle)
            table[CELLS:, column + 1] = np.cos(angle)
    angle = 2 * np.pi * np.arange(LON)[:, None] * t[None, :] / NLON
    twiddle = np.stack([np.cos(angle), np.sin(angle)]).astype(np.float32)
    geometry = np.zeros((5, 8, 128), np.float32)
    for chunk in range(5):
        for lane in range(128):
            r = 2 * chunk + lane // HALF
            if r < ROWS:
                theta = np.pi * (ROWS * (lane % HALF) + r + 0.5) / NLAT
                log_sine = np.log2(np.sin(theta))
                coarse = np.round(log_sine * 1024) / 1024
                geometry[:4, chunk, lane] = np.cos(theta), coarse, log_sine - coarse, 1.0
    weights = np.zeros((HALF, 128), np.float32)
    for r in range(ROWS):
        theta = np.pi * (ROWS * np.arange(HALF) + r + 0.5) / NLAT
        cell = np.sin(theta) * (np.pi / NLAT) * (2 * np.pi / NLON)
        weights[:, 10 * r : 10 * r + 10] = cell[:, None]
    first = [
        (0.5 * (math.lgamma(m + 1.5) - math.lgamma(1.5) - math.lgamma(m + 1.0)) - 0.5 * math.log(4 * math.pi))
        / math.log(2)
        for m in range(MODES)
    ]
    geometry[4, :SLOTS] = np.reshape(first, (SLOTS, DEV))
    twiddle = twiddle.reshape(2, LON, 2, 128).transpose(0, 2, 1, 3).reshape(4 * LON, 128)
    parts = [table.astype(np.float32), twiddle, geometry.reshape(40, 128), weights]
    return np.concatenate(parts)


def split(x):
    high = x.astype(bf16)
    return high, (x - high.astype(f32)).astype(bf16)


def cosine(n):
    return math.cos(math.pi * (n % 16) / 8)


def sine(n):
    return math.sin(math.pi * (n % 16) / 8)


def combine(terms):
    total = None
    for value, factor in terms:
        if abs(factor) < 1e-9:
            continue
        if abs(factor - 1) < 1e-9:
            term, negative = value, False
        elif abs(factor + 1) < 1e-9:
            term, negative = value, True
        else:
            term, negative = value * factor, False
        if total is None:
            total = -term if negative else term
        else:
            total = total - term if negative else total + term
    return 0.0 if total is None else total


def kernel(
    h_hbm, resp_hbm, fixed_hbm, o_ref,
    h_ref, resp_ref, table_ref, tw_ref, geo_ref, wt_ref,
    send_a, recv_a, zs, osc, send_b, recv_b, coef_a, coef_c, tall, phi, plo, phi_t, plo_t, fold, send_c, recv_c, vs, send_d, recv_d,
    ssem, rsem, lsem,
):
    loads = [
        pltpu.make_async_copy(source, target, lsem.at[n])
        for n, (source, target) in enumerate(
            [
                (h_hbm, h_ref),
                (fixed_hbm.at[pl.ds(576, 40)], geo_ref),
                (fixed_hbm.at[pl.ds(512, 64)], tw_ref),
                (fixed_hbm.at[pl.ds(0, 512)], table_ref),
                (fixed_hbm.at[pl.ds(616, 64)], wt_ref),
                (resp_hbm, resp_ref.at[pl.ds(0, SLOTS)]),
            ]
        )
    ]
    resp_ref[...] = jnp.zeros((8, 128), f32)
    for load in loads:
        load.start()
    lon = lax.axis_index("lon")
    lat = lax.axis_index("lat")
    me = lat * LON + lon
    south = lat // (LAT // 2)
    barrier = pltpu.get_barrier_semaphore()

    y, z, core = lat // 2, (lon // 2) % 4, lon % 2
    x_low = lon // 8
    x_all = (lat % 2) * 2 + x_low
    at_y = [((y + d) % 4) * 2 for d in range(4)]
    at_x = [(x_all + d) % 4 for d in range(4)]
    at_x = [(v // 2, (v % 2) * 8) for v in at_x]
    at_low = [((x_low + d) % 2) * 8 for d in range(2)]
    at_z = [((z + d) % 4) * 2 for d in range(4)]
    at_core = [core, 1 - core]
    everyone = [(at_y[dy] + at_x[dx][0], at_x[dx][1] + at_z[dz] + at_core[dc]) for dy, dx, dz, dc in FAR]
    row_peers = [at_low[dx] + at_z[dz] + at_core[dc] for dx, dz, dc in FAR_LON]

    def place(a, b):
        p = a * LON + b
        return jnp.where(a < LAT // 2, p, DEV + HALF - 1 - p)

    greeted = [(lat, b) for b in row_peers]
    x_high = lat % 2
    same, mirror = lon, (1 - x_low) * 8 + z * 2 + core
    greeted += [(at_y[d] + 1 - x_high, mirror) for d in (2, 1, 3, 0)] + [(at_y[d] + x_high, same) for d in (2, 1, 3)]
    for a, b in greeted:
        pl.semaphore_signal(barrier, inc=1, device_id={"lat": a, "lon": b})

    loads[0].wait()

    def stage(block, carry):
        for r in range(ROWS):
            source = jnp.where(south == 1, ROWS - 1 - r, r)
            line = h_ref[pl.ds(ROWS * block + source, 1), :]
            send_a[0, block, r] = line[:, :128]
            send_a[1, block, r] = line[:, 128:]
        return carry

    lax.fori_loop(0, LON, stage, 0)

    for i in range(SLOTS):
        def coefficients(block, carry, i=i):
            row = block * 32
            m = (DEV * i + me).astype(f32)
            k = (row + lax.broadcasted_iota(jnp.int32, (32, 128), 0)).astype(f32)
            k1 = k + 1.0
            l2 = 2.0 * (m + k1)
            squared = (l2 * l2 - 1.0) / (k1 * (2.0 * m + k1))
            below = l2 - 2.0
            ratio = k * (2.0 * m + k) / jnp.maximum(below * below - 1.0, 1.0)
            start = pl.multiple_of(STARTS[i] + row, 8)
            coef_a[pl.ds(start, 32), :] = jnp.sqrt(squared)
            coef_c[pl.ds(start, 32), :] = jnp.sqrt(squared * ratio)
            return carry

        lax.fori_loop(0, (MODES - DEV * i) // 32, coefficients, 0)

    pl.semaphore_wait(barrier, len(greeted))

    def exchange_lon(send, recv, which):
        for b in row_peers:
            pltpu.make_async_remote_copy(
                send.at[b], recv.at[lon], ssem.at[which], rsem.at[which], device_id={"lat": lat, "lon": b}
            ).start()
        recv[lon] = send[lon]

    def finish(send, recv, which, count):
        every = pltpu.make_async_remote_copy(
            send.at[pl.ds(0, count)], recv.at[pl.ds(0, count)], ssem.at[which], rsem.at[which],
            device_id={"lat": lat, "lon": row_peers[0]},
        )
        every.wait_send()
        every.wait_recv()

    for side in range(2):
        exchange_lon(send_a.at[side], recv_a.at[side], side)

    loads[1].wait()
    x = geo_ref[0:8, :]
    starts = pltpu.roll(geo_ref[32:40, :], lax.rem(DEV - me, DEV), axis=1)
    state = []
    for i in range(SLOTS):
        m = (DEV * i + me).astype(f32)
        coarse = m * geo_ref[8:16, :]
        fine = m * geo_ref[16:24, :] + jnp.broadcast_to(starts[i : i + 1, 0:1], (8, 128))
        count = jnp.maximum(jnp.ceil((-84.0 - (coarse + fine)) * (1.0 / 64.0)), 0.0)
        value = jnp.exp2((coarse + 64.0 * count) + fine) * geo_ref[24:32, :]
        state.append((jnp.zeros_like(value), value, count))

    for section in range(SLOTS):
        active = SLOTS - section

        def steps(block, carry, section=section, active=active):
            new = []
            for i in range(active):
                earlier, latest, count = carry[i]
                base = STARTS[i] + section * DEV
                row = pl.multiple_of(base + block * 8, 8)
                a8 = coef_a[pl.ds(row, 8), :]
                c8 = coef_c[pl.ds(row, 8), :]
                seen = jnp.where(count == 0.0, 1.0, 0.0)
                for u in range(8):
                    tall[pl.ds(pl.multiple_of((row + u) * 8, 8), 8), :] = latest * seen
                    following = (a8[u : u + 1, :] * x) * latest - c8[u : u + 1, :] * earlier
                    earlier, latest = latest, following
                large = jnp.logical_and(jnp.abs(latest) > 2.0**-20, count > 0.0)
                factor = jnp.where(large, 2.0**-64, 1.0)
                new.append((earlier * factor, latest * factor, count - jnp.where(large, 1.0, 0.0)))
            return tuple(new)

        state = list(lax.fori_loop(0, DEV // 8, steps, tuple(state[:active])))

    loads[2].wait()
    for side in range(2):
        lanes = slice(side * 128, side * 128 + 128)
        finish(send_a.at[side], recv_a.at[side], side, LON - 1)
        d = [recv_a[side, b, :, 0, :] for b in range(LON)]
        even = {b: d[b] + d[16 - b] for b in range(1, 8)}
        odd = {b: d[b] - d[16 - b] for b in range(1, 8)}
        real = [None] * 9
        imag = [None] * 9
        for rho in range(5):
            a = combine(
                [(d[0], 1.0), (d[8], 1.0 - 2.0 * (rho % 2))] + [(even[b], cosine(rho * b)) for b in (2, 4, 6)]
            )
            b_ = combine([(even[b], cosine(rho * b)) for b in (1, 3, 5, 7)])
            e = combine([(odd[b], -sine(rho * b)) for b in (2, 4, 6)])
            c = combine([(odd[b], -sine(rho * b)) for b in (1, 3, 5, 7)])
            real[rho], real[8 - rho] = a + b_, a - b_
            imag[rho], imag[8 - rho] = c + e, c - e
        for rho in range(LON):
            tc = tw_ref[side * LON + rho : side * LON + rho + 1, :]
            ts = tw_ref[(2 + side) * LON + rho : (2 + side) * LON + rho + 1, :]
            if rho % 8 == 0:
                zre, zim = real[rho] * tc, -(real[rho] * ts)
            elif rho < 8:
                zre, zim = real[rho] * tc + imag[rho] * ts, imag[rho] * tc - real[rho] * ts
            else:
                yre, yim = real[16 - rho], imag[16 - rho]
                zre, zim = yre * tc - yim * ts, -(yim * tc) - yre * ts
            zs[rho, 0:ROWS, lanes] = zre
            zs[rho, 0:ROWS, CELLS + side * 128 : CELLS + side * 128 + 128] = zim

    loads[3].wait()
    zh, zl = split(zs[...].reshape(LON * 16, 2 * CELLS))
    thi, tlo = split(table_ref[...])
    nn = (((1,), (0,)), ((), ()))
    nt = (((1,), (1,)), ((), ()))

    def product(high, low, other_high, other_low, dims):
        count = high.shape[0]
        both = lax.dot_general(jnp.concatenate([high, low], axis=0), other_high, dims, preferred_element_type=f32)
        return both[:count] + both[count:] + lax.dot_general(high, other_low, dims, preferred_element_type=f32)

    osc[...] = product(zh, zl, thi, tlo, nn)

    lane = lax.broadcasted_iota(jnp.int32, (LON, 128), 1)
    packed = [jnp.zeros((LON, 128), f32) for _ in range(LAT)]
    for r in range(ROWS):
        value = osc[pl.ds(r, LON, stride=16), :]
        mine = jnp.logical_and(lane >= 10 * r, lane < 10 * r + 10)
        for g in range(LAT):
            shift = (10 * (r - g)) % 128
            moved = pltpu.roll(value, shift, axis=1) if shift else value
            packed[g] = jnp.where(mine, moved, packed[g])
    for g in range(LAT):
        send_b[g * LON : (g + 1) * LON, :] = packed[g]

    def exchange_all(send, recv, which, source, target):
        for a, b in everyone:
            pltpu.make_async_remote_copy(
                send.at[pl.ds(source(a, b), 1)], recv.at[pl.ds(target, 1)], ssem.at[which], rsem.at[which],
                device_id={"lat": a, "lon": b},
            ).start()
        recv[pl.ds(target, 1), :] = send[pl.ds(source(lat, lon), 1), :]

    exchange_all(send_b, recv_b, 2, lambda a, b: a * LON + b, place(lat, lon))

    def halves(block, carry):
        row = pl.multiple_of(block * 128, 128)
        for j in range(5):
            value = tall[pl.ds(row * 8 + j, 128, stride=8), :]
            high, low = split(value)
            phi[pl.ds(row, 128), j * 128 : (j + 1) * 128] = high
            plo[pl.ds(row, 128), j * 128 : (j + 1) * 128] = low
            high, low = high.T, low.T
            phi_t[j * 128 : (j + 1) * 128, pl.ds(row, 128)] = high
            plo_t[j * 128 : (j + 1) * 128, pl.ds(row, 128)] = low
        return carry

    lax.fori_loop(0, TALL // 128, halves, 0)

    loads[4].wait()
    loads[5].wait()
    turned = pltpu.roll(resp_ref[...], lax.rem(DEV - me, DEV), axis=1)
    within = lax.broadcasted_iota(jnp.int32, (SLOTS, 128), 1) < DEV - me
    shifted = jnp.where(within, turned[0:SLOTS], turned[1 : SLOTS + 1])
    response = jnp.concatenate(
        [shifted[q : q + 1] for i in range(SLOTS) for q in range(i, SLOTS)], axis=1
    )
    first = jnp.where(jnp.logical_and(lax.broadcasted_iota(jnp.int32, (1, TALL), 1) < MODES, me == 0), 1.0, 2.0)
    response = response * first
    row = lax.broadcasted_iota(jnp.int32, (32, TALL), 0)
    column = lax.broadcasted_iota(jnp.int32, (32, TALL), 1)
    slot = jnp.zeros((32, TALL), jnp.int32)
    for i in range(1, SLOTS):
        slot = slot + jnp.where(column >= STARTS[i], 1, 0)
    wanted = 2 * slot + 16 * (column & 1)
    keep = jnp.logical_or(row == wanted, row == wanted + 1)
    gain = jnp.where(keep, response, 0.0)

    finish(send_b, recv_b, 2, DEV - 1)

    north = recv_b[0:HALF, :]
    southern = recv_b[HALF:DEV, :]
    weights = wt_ref[...]
    folded = jnp.concatenate([(north + southern) * weights, (north - southern) * weights], axis=0)
    fold[...] = folded.T
    left = lax.broadcasted_iota(jnp.int32, (10, 128), 1) < HALF
    evens = []
    odds = []
    for j in range(5):
        first_row = fold[20 * j : 20 * j + 10, :]
        if j < 4:
            second_row = fold[20 * j + 10 : 20 * j + 20, :]
        else:
            second_row = jnp.zeros((10, 128), f32)
        evens.append(jnp.where(left, first_row, pltpu.roll(second_row, HALF, axis=1)))
        odds.append(jnp.where(left, pltpu.roll(first_row, HALF, axis=1), second_row))
    pad = jnp.zeros((6, WIDE), f32)
    lhs = jnp.concatenate([jnp.concatenate(evens, axis=1), pad, jnp.concatenate(odds, axis=1), pad], axis=0)
    lh, ll = split(lhs)
    sh, sl = split(product(lh, ll, phi_t[...], plo_t[...], nn) * gain)
    synthesis = product(sh, sl, phi[...], plo[...], nn)
    fold[...] = jnp.zeros((128, 128), f32)
    for j in range(5):
        e = synthesis[0:10, j * 128 : (j + 1) * 128]
        o = synthesis[16:26, j * 128 : (j + 1) * 128]
        n, s = e + o, e - o
        fold[20 * j : 20 * j + 10, :] = jnp.where(left, n, pltpu.roll(s, HALF, axis=1))
        if j < 4:
            fold[20 * j + 10 : 20 * j + 20, :] = jnp.where(left, pltpu.roll(n, HALF, axis=1), s)
    send_c[...] = fold[...].T

    exchange_all(send_c, recv_c, 3, place, me)
    finish(send_c, recv_c, 3, DEV - 1)

    pieces = [recv_c[g * LON : (g + 1) * LON, :] for g in range(LAT)]
    gathered = []
    for r in range(ROWS):
        value = jnp.zeros((LON, 128), f32)
        for g in range(LAT):
            mine = jnp.logical_and(lane >= 10 * g, lane < 10 * g + 10)
            shift = (10 * (g - r)) % 128
            moved = pltpu.roll(pieces[g], shift, axis=1) if shift else pieces[g]
            value = jnp.where(mine, moved, value)
        gathered.append(value)
    gh, gl = split(jnp.concatenate(gathered, axis=0))
    inverse = product(gh, gl, thi, tlo, nt)
    for c in range(4):
        vs[c] = inverse[:, c * 128 : (c + 1) * 128]

    for side in range(2):
        lanes = slice(side * 128, side * 128 + 128)
        real = []
        imag = []
        for rho in range(LON):
            tc = tw_ref[side * LON + rho : side * LON + rho + 1, :]
            ts = tw_ref[(2 + side) * LON + rho : (2 + side) * LON + rho + 1, :]
            vre = vs[side, pl.ds(rho, ROWS, stride=16), :]
            vim = vs[2 + side, pl.ds(rho, ROWS, stride=16), :]
            real.append(vre * tc - vim * ts)
            imag.append(None if rho % 8 == 0 else vre * ts + vim * tc)
        ure = {rho: real[rho] + real[16 - rho] for rho in range(1, 8)}
        uim = {rho: imag[rho] - imag[16 - rho] for rho in range(1, 8)}
        def put(b, value, side=side):
            for r in range(ROWS):
                target = ROWS * b + jnp.where(south == 1, ROWS - 1 - r, r)
                send_d[side, pl.ds(target, 1), :] = value[r : r + 1]

        for b in range(5):
            ge = combine(
                [(real[0], 1.0), (real[8], 1.0 - 2.0 * (b % 2))] + [(ure[q], cosine(q * b)) for q in (2, 4, 6)]
            )
            go = combine([(ure[q], cosine(q * b)) for q in (1, 3, 5, 7)])
            he = combine([(uim[q], sine(q * b)) for q in (2, 4, 6)])
            ho = combine([(uim[q], sine(q * b)) for q in (1, 3, 5, 7)])
            put(b, (ge + go) - (he + ho))
            if b > 0:
                put(16 - b, (ge + go) + (he + ho))
            if b < 4:
                put(8 - b, (ge - go) - (ho - he))
                if b > 0:
                    put(8 + b, (ge - go) + (ho - he))
        for b in row_peers:
            pltpu.make_async_remote_copy(
                send_d.at[side, pl.ds(ROWS * b, ROWS)], recv_d.at[side, pl.ds(ROWS * lon, ROWS)],
                ssem.at[4 + side], rsem.at[4 + side], device_id={"lat": lat, "lon": b},
            ).start()
        for r in range(ROWS):
            recv_d[side, pl.ds(ROWS * lon + r, 1), :] = send_d[side, pl.ds(ROWS * lon + r, 1), :]

    for side in range(2):
        lanes = slice(side * 128, side * 128 + 128)
        finish(send_d.at[side], recv_d.at[side], 4 + side, ROWS * (LON - 1))
        o_ref[:, lanes] = recv_d[side]


def shards(height, response):
    fixed = constants()
    hbm = pl.BlockSpec(memory_space=pltpu.HBM)
    blocks = pltpu.VMEM((2, LON, ROWS, 1, 128), f32)
    rows = pltpu.VMEM((DEV, 128), f32)
    out = pl.pallas_call(
        kernel,
        out_shape=jax.ShapeDtypeStruct((NLAT // LAT, CELLS), f32),
        in_specs=[hbm] * 3,
        out_specs=pl.BlockSpec(memory_space=pltpu.VMEM),
        scratch_shapes=[
            pltpu.VMEM((NLAT // LAT, CELLS), f32),
            pltpu.VMEM((8, 128), f32),
            pltpu.VMEM((2 * CELLS, 128), f32),
            pltpu.VMEM((4 * LON, 128), f32),
            pltpu.VMEM((40, 128), f32),
            pltpu.VMEM((HALF, 128), f32),
            blocks,
            blocks,
            pltpu.VMEM((LON, 16, 2 * CELLS), f32),
            pltpu.VMEM((LON * 16, 128), f32),
            rows,
            rows,
            pltpu.VMEM((TALL, 128), f32),
            pltpu.VMEM((TALL, 128), f32),
            pltpu.VMEM((TALL * 8, 128), f32),
            pltpu.VMEM((TALL, WIDE), bf16),
            pltpu.VMEM((TALL, WIDE), bf16),
            pltpu.VMEM((WIDE, TALL), bf16),
            pltpu.VMEM((WIDE, TALL), bf16),
            pltpu.VMEM((128, 128), f32),
            rows,
            rows,
            pltpu.VMEM((4, ROWS * LON, 128), f32),
            pltpu.VMEM((2, NLAT // LAT, 128), f32),
            pltpu.VMEM((2, NLAT // LAT, 128), f32),
            pltpu.SemaphoreType.DMA((6,)),
            pltpu.SemaphoreType.DMA((6,)),
            pltpu.SemaphoreType.DMA((6,)),
        ],
        compiler_params=pltpu.CompilerParams(
            collective_id=0, has_side_effects=True, vmem_limit_bytes=40 * 1024 * 1024
        ),
    )(
        pltpu.with_memory_space_constraint(height.reshape(NLAT // LAT, CELLS), pltpu.HBM),
        pltpu.with_memory_space_constraint(response.reshape(SLOTS, 128), pltpu.HBM),
        pltpu.with_memory_space_constraint(jnp.asarray(fixed), pltpu.HBM),
    )
    return out.reshape(height.shape)


def solution(mesh):
    placed = (P(None, "lat", "lon"), P())
    return jax.shard_map(
        shards, mesh=mesh, in_specs=placed, out_specs=P(None, "lat", "lon"), check_vma=False
    )
```

```python
import math

import jax
import jax.numpy as jnp
import numpy as np
from jax import lax
from jax.experimental import pallas as pl
from jax.experimental.pallas import tpu as pltpu
from jax.sharding import PartitionSpec as P

NLAT = 1152
NLON = 4096
MODES = 640
LON = 16
LAT = 8
DEV = LON * LAT
ROWS = NLAT // DEV
CELLS = NLON // LON
SLOTS = MODES // DEV
HALF = DEV // 2
STARTS = [sum(MODES - DEV * t for t in range(i)) for i in range(SLOTS)]
TALL = sum(MODES - DEV * t for t in range(SLOTS))
WIDE = 640
HOPS = (0, 1, 2, 1)
FAR = sorted(
    [(dy, dx, dz, dc) for dy in range(4) for dx in range(4) for dz in range(4) for dc in range(2)],
    key=lambda o: (-HOPS[o[0]] - HOPS[o[1]] - HOPS[o[2]], -o[3]),
)[: DEV - 1]
FAR_LON = sorted(
    [(dx, dz, dc) for dx in range(2) for dz in range(4) for dc in range(2)],
    key=lambda o: (-o[0] - HOPS[o[1]], -o[2]),
)[: LON - 1]
bf16 = jnp.bfloat16
f32 = jnp.float32


def constants():
    t = np.arange(CELLS)
    table = np.zeros((2 * CELLS, 128))
    for g in range(LAT):
        for i in range(SLOTS):
            angle = 2 * np.pi * ((g + LAT * i) * t % CELLS) / CELLS
            column = (g * SLOTS + i) * 2
            table[:CELLS, column] = np.cos(angle)
            table[CELLS:, column] = np.sin(angle)
            table[:CELLS, column + 1] = -np.sin(angle)
            table[CELLS:, column + 1] = np.cos(angle)
    angle = 2 * np.pi * np.arange(LON)[:, None] * t[None, :] / NLON
    twiddle = np.stack([np.cos(angle), np.sin(angle)]).astype(np.float32)
    geometry = np.zeros((5, 8, 128), np.float32)
    for chunk in range(5):
        for lane in range(128):
            r = 2 * chunk + lane // HALF
            if r < ROWS:
                theta = np.pi * (ROWS * (lane % HALF) + r + 0.5) / NLAT
                log_sine = np.log2(np.sin(theta))
                coarse = np.round(log_sine * 1024) / 1024
                geometry[:4, chunk, lane] = np.cos(theta), coarse, log_sine - coarse, 1.0
    weights = np.zeros((HALF, 128), np.float32)
    for r in range(ROWS):
        theta = np.pi * (ROWS * np.arange(HALF) + r + 0.5) / NLAT
        cell = np.sin(theta) * (np.pi / NLAT) * (2 * np.pi / NLON)
        weights[:, 10 * r : 10 * r + 10] = cell[:, None]
    first = [
        (0.5 * (math.lgamma(m + 1.5) - math.lgamma(1.5) - math.lgamma(m + 1.0)) - 0.5 * math.log(4 * math.pi))
        / math.log(2)
        for m in range(MODES)
    ]
    geometry[4, :SLOTS] = np.reshape(first, (SLOTS, DEV))
    twiddle = twiddle.reshape(2, LON, 2, 128).transpose(0, 2, 1, 3).reshape(4 * LON, 128)
    parts = [table.astype(np.float32), twiddle, geometry.reshape(40, 128), weights]
    return np.concatenate(parts)


def split(x):
    high = x.astype(bf16)
    return high, (x - high.astype(f32)).astype(bf16)


def cosine(n):
    return math.cos(math.pi * (n % 16) / 8)


def sine(n):
    return math.sin(math.pi * (n % 16) / 8)


def combine(terms):
    total = None
    for value, factor in terms:
        if abs(factor) < 1e-9:
            continue
        if abs(factor - 1) < 1e-9:
            term, negative = value, False
        elif abs(factor + 1) < 1e-9:
            term, negative = value, True
        else:
            term, negative = value * factor, False
        if total is None:
            total = -term if negative else term
        else:
            total = total - term if negative else total + term
    return 0.0 if total is None else total


def kernel(
    h_hbm, resp_hbm, fixed_hbm, o_ref,
    h_ref, resp_ref, table_ref, thi_ref, tlo_ref, tw_ref, geo_ref, wt_ref,
    send_a, recv_a, zs, osc, send_b, recv_b, coef_a, coef_c, tall, phi, plo, phi_t, plo_t, fold, send_c, recv_c, vs, send_d, recv_d,
    ssem, rsem, lsem,
):
    loads = [
        pltpu.make_async_copy(source, target, lsem.at[n])
        for n, (source, target) in enumerate(
            [
                (h_hbm, h_ref),
                (fixed_hbm.at[pl.ds(576, 40)], geo_ref),
                (fixed_hbm.at[pl.ds(512, 64)], tw_ref),
                (fixed_hbm.at[pl.ds(0, 512)], table_ref),
                (fixed_hbm.at[pl.ds(616, 64)], wt_ref),
                (resp_hbm, resp_ref.at[pl.ds(0, SLOTS)]),
            ]
        )
    ]
    loads[0].start()
    lon = lax.axis_index("lon")
    lat = lax.axis_index("lat")
    me = lat * LON + lon
    south = lat // (LAT // 2)
    barrier = pltpu.get_barrier_semaphore()

    y, z, core = lat // 2, (lon // 2) % 4, lon % 2
    x_low = lon // 8
    x_all = (lat % 2) * 2 + x_low
    at_y = [((y + d) % 4) * 2 for d in range(4)]
    at_x = [(x_all + d) % 4 for d in range(4)]
    at_x = [(v // 2, (v % 2) * 8) for v in at_x]
    at_low = [((x_low + d) % 2) * 8 for d in range(2)]
    at_z = [((z + d) % 4) * 2 for d in range(4)]
    at_core = [core, 1 - core]
    everyone = [(at_y[dy] + at_x[dx][0], at_x[dx][1] + at_z[dz] + at_core[dc]) for dy, dx, dz, dc in FAR]
    row_peers = [at_low[dx] + at_z[dz] + at_core[dc] for dx, dz, dc in FAR_LON]

    def place(a, b):
        p = a * LON + b
        return jnp.where(a < LAT // 2, p, DEV + HALF - 1 - p)

    greeted = [(lat, b) for b in row_peers]
    x_high = lat % 2
    same, mirror = lon, (1 - x_low) * 8 + z * 2 + core
    greeted += [(at_y[d] + 1 - x_high, mirror) for d in (2, 1, 3, 0)] + [(at_y[d] + x_high, same) for d in (2, 1, 3)]
    for a, b in greeted:
        pl.semaphore_signal(barrier, inc=1, device_id={"lat": a, "lon": b})

    resp_ref[...] = jnp.zeros((8, 128), f32)
    for load in loads[1:]:
        load.start()
    loads[0].wait()

    def stage(block, carry):
        for r in range(ROWS):
            source = jnp.where(south == 1, ROWS - 1 - r, r)
            line = h_ref[pl.ds(ROWS * block + source, 1), :]
            send_a[0, block, r] = line[:, :128]
            send_a[1, block, r] = line[:, 128:]
        return carry

    lax.fori_loop(0, LON, stage, 0)

    for i in range(SLOTS):
        def coefficients(block, carry, i=i):
            row = block * 32
            m = (DEV * i + me).astype(f32)
            k = (row + lax.broadcasted_iota(jnp.int32, (32, 128), 0)).astype(f32)
            k1 = k + 1.0
            l2 = 2.0 * (m + k1)
            squared = (l2 * l2 - 1.0) / (k1 * (2.0 * m + k1))
            below = l2 - 2.0
            ratio = k * (2.0 * m + k) / jnp.maximum(below * below - 1.0, 1.0)
            start = pl.multiple_of(STARTS[i] + row, 8)
            coef_a[pl.ds(start, 32), :] = jnp.sqrt(squared)
            coef_c[pl.ds(start, 32), :] = jnp.sqrt(squared * ratio)
            return carry

        lax.fori_loop(0, (MODES - DEV * i) // 32, coefficients, 0)

    pl.semaphore_wait(barrier, len(greeted))

    def exchange_lon(send, recv, which):
        for b in row_peers:
            pltpu.make_async_remote_copy(
                send.at[b], recv.at[lon], ssem.at[which], rsem.at[which], device_id={"lat": lat, "lon": b}
            ).start()
        recv[lon] = send[lon]

    def finish(send, recv, which, count):
        every = pltpu.make_async_remote_copy(
            send.at[pl.ds(0, count)], recv.at[pl.ds(0, count)], ssem.at[which], rsem.at[which],
            device_id={"lat": lat, "lon": row_peers[0]},
        )
        every.wait_send()
        every.wait_recv()

    for side in range(2):
        exchange_lon(send_a.at[side], recv_a.at[side], side)

    loads[1].wait()
    x = geo_ref[0:8, :]
    starts = pltpu.roll(geo_ref[32:40, :], lax.rem(DEV - me, DEV), axis=1)
    state = []
    for i in range(SLOTS):
        m = (DEV * i + me).astype(f32)
        coarse = m * geo_ref[8:16, :]
        fine = m * geo_ref[16:24, :] + jnp.broadcast_to(starts[i : i + 1, 0:1], (8, 128))
        count = jnp.maximum(jnp.ceil((-84.0 - (coarse + fine)) * (1.0 / 64.0)), 0.0)
        value = jnp.exp2((coarse + 64.0 * count) + fine) * geo_ref[24:32, :]
        state.append((jnp.zeros_like(value), value, count))

    for section in range(SLOTS):
        active = SLOTS - section

        def steps(block, carry, section=section, active=active):
            new = []
            for i in range(active):
                earlier, latest, count = carry[i]
                base = STARTS[i] + section * DEV
                row = pl.multiple_of(base + block * 8, 8)
                a8 = coef_a[pl.ds(row, 8), :]
                c8 = coef_c[pl.ds(row, 8), :]
                seen = jnp.where(count == 0.0, 1.0, 0.0)
                for u in range(8):
                    tall[pl.ds(pl.multiple_of((row + u) * 8, 8), 8), :] = latest * seen
                    following = (a8[u : u + 1, :] * x) * latest - c8[u : u + 1, :] * earlier
                    earlier, latest = latest, following
                large = jnp.logical_and(jnp.abs(latest) > 2.0**-20, count > 0.0)
                factor = jnp.where(large, 2.0**-64, 1.0)
                new.append((earlier * factor, latest * factor, count - jnp.where(large, 1.0, 0.0)))
            return tuple(new)

        state = list(lax.fori_loop(0, DEV // 8, steps, tuple(state[:active])))

    loads[3].wait()
    thi_ref[...], tlo_ref[...] = split(table_ref[...])
    loads[2].wait()
    for side in range(2):
        lanes = slice(side * 128, side * 128 + 128)
        finish(send_a.at[side], recv_a.at[side], side, LON - 1)
        d = [recv_a[side, b, :, 0, :] for b in range(LON)]
        even = {b: d[b] + d[16 - b] for b in range(1, 8)}
        odd = {b: d[b] - d[16 - b] for b in range(1, 8)}
        real = [None] * 9
        imag = [None] * 9
        for rho in range(5):
            a = combine(
                [(d[0], 1.0), (d[8], 1.0 - 2.0 * (rho % 2))] + [(even[b], cosine(rho * b)) for b in (2, 4, 6)]
            )
            b_ = combine([(even[b], cosine(rho * b)) for b in (1, 3, 5, 7)])
            e = combine([(odd[b], -sine(rho * b)) for b in (2, 4, 6)])
            c = combine([(odd[b], -sine(rho * b)) for b in (1, 3, 5, 7)])
            real[rho], real[8 - rho] = a + b_, a - b_
            imag[rho], imag[8 - rho] = c + e, c - e
        for rho in range(LON):
            tc = tw_ref[side * LON + rho : side * LON + rho + 1, :]
            ts = tw_ref[(2 + side) * LON + rho : (2 + side) * LON + rho + 1, :]
            if rho % 8 == 0:
                zre, zim = real[rho] * tc, -(real[rho] * ts)
            elif rho < 8:
                zre, zim = real[rho] * tc + imag[rho] * ts, imag[rho] * tc - real[rho] * ts
            else:
                yre, yim = real[16 - rho], imag[16 - rho]
                zre, zim = yre * tc - yim * ts, -(yim * tc) - yre * ts
            zs[rho, 0:ROWS, lanes] = zre
            zs[rho, 0:ROWS, CELLS + side * 128 : CELLS + side * 128 + 128] = zim

    zh, zl = split(zs[...].reshape(LON * 16, 2 * CELLS))
    thi, tlo = thi_ref[...], tlo_ref[...]
    nn = (((1,), (0,)), ((), ()))
    nt = (((1,), (1,)), ((), ()))

    def product(high, low, other_high, other_low, dims):
        count = high.shape[0]
        both = lax.dot_general(jnp.concatenate([high, low], axis=0), other_high, dims, preferred_element_type=f32)
        return both[:count] + both[count:] + lax.dot_general(high, other_low, dims, preferred_element_type=f32)

    osc[0 : LON * 16, :] = product(zh, zl, thi, tlo, nn)

    lane = lax.broadcasted_iota(jnp.int32, (LON, 128), 1)
    packed = [jnp.zeros((LON, 128), f32) for _ in range(LAT)]
    for r in range(ROWS):
        value = osc[pl.ds(r, LON, stride=16), :]
        mine = jnp.logical_and(lane >= 10 * r, lane < 10 * r + 10)
        for g in range(LAT):
            shift = (10 * (r - g)) % 128
            moved = pltpu.roll(value, shift, axis=1) if shift else value
            packed[g] = jnp.where(mine, moved, packed[g])
    for g in range(LAT):
        send_b[g * LON : (g + 1) * LON, :] = packed[g]

    def exchange_all(send, recv, which, source, target):
        for a, b in everyone:
            pltpu.make_async_remote_copy(
                send.at[pl.ds(source(a, b), 1)], recv.at[pl.ds(target, 1)], ssem.at[which], rsem.at[which],
                device_id={"lat": a, "lon": b},
            ).start()
        recv[pl.ds(target, 1), :] = send[pl.ds(source(lat, lon), 1), :]

    exchange_all(send_b, recv_b, 2, lambda a, b: a * LON + b, place(lat, lon))

    def halves(block, carry):
        row = pl.multiple_of(block * 128, 128)
        for j in range(5):
            value = tall[pl.ds(row * 8 + j, 128, stride=8), :]
            high, low = split(value)
            phi[pl.ds(row, 128), j * 128 : (j + 1) * 128] = high
            plo[pl.ds(row, 128), j * 128 : (j + 1) * 128] = low
            high, low = high.T, low.T
            phi_t[j * 128 : (j + 1) * 128, pl.ds(row, 128)] = high
            plo_t[j * 128 : (j + 1) * 128, pl.ds(row, 128)] = low
        return carry

    lax.fori_loop(0, TALL // 128, halves, 0)

    loads[4].wait()
    loads[5].wait()
    turned = pltpu.roll(resp_ref[...], lax.rem(DEV - me, DEV), axis=1)
    within = lax.broadcasted_iota(jnp.int32, (SLOTS, 128), 1) < DEV - me
    shifted = jnp.where(within, turned[0:SLOTS], turned[1 : SLOTS + 1])
    response = jnp.concatenate(
        [shifted[q : q + 1] for i in range(SLOTS) for q in range(i, SLOTS)], axis=1
    )
    first = jnp.where(jnp.logical_and(lax.broadcasted_iota(jnp.int32, (1, TALL), 1) < MODES, me == 0), 1.0, 2.0)
    response = response * first
    row = lax.broadcasted_iota(jnp.int32, (32, TALL), 0)
    column = lax.broadcasted_iota(jnp.int32, (32, TALL), 1)
    slot = jnp.zeros((32, TALL), jnp.int32)
    for i in range(1, SLOTS):
        slot = slot + jnp.where(column >= STARTS[i], 1, 0)
    wanted = 2 * slot + 16 * (column & 1)
    keep = jnp.logical_or(row == wanted, row == wanted + 1)
    gain = jnp.where(keep, response, 0.0)

    finish(send_b, recv_b, 2, DEV - 1)

    north = recv_b[0:HALF, :]
    southern = recv_b[HALF:DEV, :]
    weights = wt_ref[...]
    folded = jnp.concatenate([(north + southern) * weights, (north - southern) * weights], axis=0)
    fold[...] = folded.T
    left = lax.broadcasted_iota(jnp.int32, (10, 128), 1) < HALF
    evens = []
    odds = []
    for j in range(5):
        first_row = fold[20 * j : 20 * j + 10, :]
        if j < 4:
            second_row = fold[20 * j + 10 : 20 * j + 20, :]
        else:
            second_row = jnp.zeros((10, 128), f32)
        evens.append(jnp.where(left, first_row, pltpu.roll(second_row, HALF, axis=1)))
        odds.append(jnp.where(left, pltpu.roll(first_row, HALF, axis=1), second_row))
    pad = jnp.zeros((6, WIDE), f32)
    lhs = jnp.concatenate([jnp.concatenate(evens, axis=1), pad, jnp.concatenate(odds, axis=1), pad], axis=0)
    lh, ll = split(lhs)
    used = ROWS * HALF
    sh, sl = split(product(lh[:, :used], ll[:, :used], phi_t[:used], plo_t[:used], nn) * gain)
    synthesis = product(sh, sl, phi[...], plo[...], nn)
    fold[...] = jnp.zeros((128, 128), f32)
    for j in range(5):
        e = synthesis[0:10, j * 128 : (j + 1) * 128]
        o = synthesis[16:26, j * 128 : (j + 1) * 128]
        n, s = e + o, e - o
        fold[20 * j : 20 * j + 10, :] = jnp.where(left, n, pltpu.roll(s, HALF, axis=1))
        if j < 4:
            fold[20 * j + 10 : 20 * j + 20, :] = jnp.where(left, pltpu.roll(n, HALF, axis=1), s)
    send_c[...] = fold[...].T

    exchange_all(send_c, recv_c, 3, place, me)
    finish(send_c, recv_c, 3, DEV - 1)

    pieces = [recv_c[g * LON : (g + 1) * LON, :] for g in range(LAT)]
    gathered = []
    for r in range(ROWS):
        value = jnp.zeros((LON, 128), f32)
        for g in range(LAT):
            mine = jnp.logical_and(lane >= 10 * g, lane < 10 * g + 10)
            shift = (10 * (g - r)) % 128
            moved = pltpu.roll(pieces[g], shift, axis=1) if shift else pieces[g]
            value = jnp.where(mine, moved, value)
        gathered.append(value)
    gh, gl = split(jnp.concatenate(gathered, axis=0))
    inverse = product(gh, gl, thi, tlo, nt)
    for c in range(4):
        vs[c, 0 : ROWS * LON, :] = inverse[:, c * 128 : (c + 1) * 128]

    for side in range(2):
        lanes = slice(side * 128, side * 128 + 128)
        real = []
        imag = []
        for rho in range(LON):
            tc = tw_ref[side * LON + rho : side * LON + rho + 1, :]
            ts = tw_ref[(2 + side) * LON + rho : (2 + side) * LON + rho + 1, :]
            vre = vs[side, pl.ds(rho, ROWS, stride=16), :]
            vim = vs[2 + side, pl.ds(rho, ROWS, stride=16), :]
            real.append(vre * tc - vim * ts)
            imag.append(None if rho % 8 == 0 else vre * ts + vim * tc)
        ure = {rho: real[rho] + real[16 - rho] for rho in range(1, 8)}
        uim = {rho: imag[rho] - imag[16 - rho] for rho in range(1, 8)}
        def put(b, value, side=side):
            for r in range(ROWS):
                target = ROWS * b + jnp.where(south == 1, ROWS - 1 - r, r)
                send_d[side, pl.ds(target, 1), :] = value[r : r + 1]

        for b in range(5):
            ge = combine(
                [(real[0], 1.0), (real[8], 1.0 - 2.0 * (b % 2))] + [(ure[q], cosine(q * b)) for q in (2, 4, 6)]
            )
            go = combine([(ure[q], cosine(q * b)) for q in (1, 3, 5, 7)])
            he = combine([(uim[q], sine(q * b)) for q in (2, 4, 6)])
            ho = combine([(uim[q], sine(q * b)) for q in (1, 3, 5, 7)])
            put(b, (ge + go) - (he + ho))
            if b > 0:
                put(16 - b, (ge + go) + (he + ho))
            if b < 4:
                put(8 - b, (ge - go) - (ho - he))
                if b > 0:
                    put(8 + b, (ge - go) + (ho - he))
        for b in row_peers:
            pltpu.make_async_remote_copy(
                send_d.at[side, pl.ds(ROWS * b, ROWS)], recv_d.at[side, pl.ds(ROWS * lon, ROWS)],
                ssem.at[4 + side], rsem.at[4 + side], device_id={"lat": lat, "lon": b},
            ).start()
        for r in range(ROWS):
            recv_d[side, pl.ds(ROWS * lon + r, 1), :] = send_d[side, pl.ds(ROWS * lon + r, 1), :]

    for side in range(2):
        lanes = slice(side * 128, side * 128 + 128)
        finish(send_d.at[side], recv_d.at[side], 4 + side, ROWS * (LON - 1))
        o_ref[:, lanes] = recv_d[side]


def shards(height, response):
    fixed = constants()
    hbm = pl.BlockSpec(memory_space=pltpu.HBM)
    blocks = pltpu.VMEM((2, LON, ROWS, 1, 128), f32)
    rows = pltpu.VMEM((DEV, 128), f32)
    out = pl.pallas_call(
        kernel,
        out_shape=jax.ShapeDtypeStruct((NLAT // LAT, CELLS), f32),
        in_specs=[hbm] * 3,
        out_specs=pl.BlockSpec(memory_space=pltpu.VMEM),
        scratch_shapes=[
            pltpu.VMEM((NLAT // LAT, CELLS), f32),
            pltpu.VMEM((8, 128), f32),
            pltpu.VMEM((2 * CELLS, 128), f32),
            pltpu.VMEM((2 * CELLS, 128), bf16),
            pltpu.VMEM((2 * CELLS, 128), bf16),
            pltpu.VMEM((4 * LON, 128), f32),
            pltpu.VMEM((40, 128), f32),
            pltpu.VMEM((HALF, 128), f32),
            blocks,
            blocks,
            pltpu.VMEM((LON, 16, 2 * CELLS), f32),
            pltpu.VMEM((LON * 16 + 16, 128), f32),
            rows,
            rows,
            pltpu.VMEM((TALL, 128), f32),
            pltpu.VMEM((TALL, 128), f32),
            pltpu.VMEM((TALL * 8 + 8, 128), f32),
            pltpu.VMEM((TALL, WIDE), bf16),
            pltpu.VMEM((TALL, WIDE), bf16),
            pltpu.VMEM((WIDE, TALL), bf16),
            pltpu.VMEM((WIDE, TALL), bf16),
            pltpu.VMEM((128, 128), f32),
            rows,
            rows,
            pltpu.VMEM((4, 16 * LON + 16, 128), f32),
            pltpu.VMEM((2, NLAT // LAT, 128), f32),
            pltpu.VMEM((2, NLAT // LAT, 128), f32),
            pltpu.SemaphoreType.DMA((6,)),
            pltpu.SemaphoreType.DMA((6,)),
            pltpu.SemaphoreType.DMA((6,)),
        ],
        compiler_params=pltpu.CompilerParams(
            collective_id=0, has_side_effects=True, vmem_limit_bytes=40 * 1024 * 1024
        ),
    )(
        pltpu.with_memory_space_constraint(height.reshape(NLAT // LAT, CELLS), pltpu.HBM),
        pltpu.with_memory_space_constraint(response.reshape(SLOTS, 128), pltpu.HBM),
        pltpu.with_memory_space_constraint(jnp.asarray(fixed), pltpu.HBM),
    )
    return out.reshape(height.shape)


def solution(mesh):
    placed = (P(None, "lat", "lon"), P())
    return jax.shard_map(
        shards, mesh=mesh, in_specs=placed, out_specs=P(None, "lat", "lon"), check_vma=False
    )
```

```python
import math

import jax
import jax.numpy as jnp
import numpy as np
from jax import lax
from jax.experimental import pallas as pl
from jax.experimental.pallas import tpu as pltpu
from jax.sharding import PartitionSpec as P

NLAT = 1152
NLON = 4096
MODES = 640
LON = 16
LAT = 8
DEV = LON * LAT
ROWS = NLAT // DEV
CELLS = NLON // LON
SLOTS = MODES // DEV
HALF = DEV // 2
STARTS = [sum(MODES - DEV * t for t in range(i)) for i in range(SLOTS)]
TALL = sum(MODES - DEV * t for t in range(SLOTS))
WIDE = 640
HOPS = (0, 1, 2, 1)
FAR = sorted(
    [(dy, dx, dz, dc) for dy in range(4) for dx in range(4) for dz in range(4) for dc in range(2)],
    key=lambda o: (-HOPS[o[0]] - HOPS[o[1]] - HOPS[o[2]], -o[3]),
)[: DEV - 1]
FAR_LON = sorted(
    [(dx, dz, dc) for dx in range(2) for dz in range(4) for dc in range(2)],
    key=lambda o: (-o[0] - HOPS[o[1]], -o[2]),
)[: LON - 1]
bf16 = jnp.bfloat16
f32 = jnp.float32


def constants():
    t = np.arange(CELLS)
    table = np.zeros((2 * CELLS, 128))
    for g in range(LAT):
        for i in range(SLOTS):
            angle = 2 * np.pi * ((g + LAT * i) * t % CELLS) / CELLS
            column = (g * SLOTS + i) * 2
            table[:CELLS, column] = np.cos(angle)
            table[CELLS:, column] = np.sin(angle)
            table[:CELLS, column + 1] = -np.sin(angle)
            table[CELLS:, column + 1] = np.cos(angle)
    angle = 2 * np.pi * np.arange(LON)[:, None] * t[None, :] / NLON
    twiddle = np.stack([np.cos(angle), np.sin(angle)]).astype(np.float32)
    geometry = np.zeros((5, 8, 128), np.float32)
    for chunk in range(5):
        for lane in range(128):
            r = 2 * chunk + lane // HALF
            if r < ROWS:
                theta = np.pi * (ROWS * (lane % HALF) + r + 0.5) / NLAT
                log_sine = np.log2(np.sin(theta))
                coarse = np.round(log_sine * 1024) / 1024
                geometry[:4, chunk, lane] = np.cos(theta), coarse, log_sine - coarse, 1.0
    weights = np.zeros((HALF, 128), np.float32)
    for r in range(ROWS):
        theta = np.pi * (ROWS * np.arange(HALF) + r + 0.5) / NLAT
        cell = np.sin(theta) * (np.pi / NLAT) * (2 * np.pi / NLON)
        weights[:, 10 * r : 10 * r + 10] = cell[:, None]
    first = [
        (0.5 * (math.lgamma(m + 1.5) - math.lgamma(1.5) - math.lgamma(m + 1.0)) - 0.5 * math.log(4 * math.pi))
        / math.log(2)
        for m in range(MODES)
    ]
    geometry[4, :SLOTS] = np.reshape(first, (SLOTS, DEV))
    twiddle = twiddle.reshape(2, LON, 2, 128).transpose(0, 2, 1, 3).reshape(4 * LON, 128)
    parts = [table.astype(np.float32), twiddle, geometry.reshape(40, 128), weights]
    return np.concatenate(parts)


def split(x):
    high = x.astype(bf16)
    return high, (x - high.astype(f32)).astype(bf16)


def cosine(n):
    return math.cos(math.pi * (n % 16) / 8)


def sine(n):
    return math.sin(math.pi * (n % 16) / 8)


def combine(terms):
    total = None
    for value, factor in terms:
        if abs(factor) < 1e-9:
            continue
        if abs(factor - 1) < 1e-9:
            term, negative = value, False
        elif abs(factor + 1) < 1e-9:
            term, negative = value, True
        else:
            term, negative = value * factor, False
        if total is None:
            total = -term if negative else term
        else:
            total = total - term if negative else total + term
    return 0.0 if total is None else total


def kernel(
    h_hbm, resp_hbm, fixed_hbm, o_ref,
    h_ref, resp_ref, table_ref, thi_ref, tlo_ref, tw_ref, geo_ref, wt_ref,
    send_a, recv_a, zs, osc, send_b, recv_b, coef_a, coef_c, tall, phi, plo, phi_t, plo_t, fold, send_c, recv_c, vs, send_d, recv_d,
    ssem, rsem, lsem,
):
    loads = [
        pltpu.make_async_copy(source, target, lsem.at[n])
        for n, (source, target) in enumerate(
            [
                (h_hbm, h_ref),
                (fixed_hbm.at[pl.ds(576, 40)], geo_ref),
                (fixed_hbm.at[pl.ds(512, 64)], tw_ref),
                (fixed_hbm.at[pl.ds(0, 512)], table_ref),
                (fixed_hbm.at[pl.ds(616, 64)], wt_ref),
                (resp_hbm, resp_ref.at[pl.ds(0, SLOTS)]),
            ]
        )
    ]
    loads[0].start()
    lon = lax.axis_index("lon")
    lat = lax.axis_index("lat")
    me = lat * LON + lon
    south = lat // (LAT // 2)
    barrier = pltpu.get_barrier_semaphore()

    y, z, core = lat // 2, (lon // 2) % 4, lon % 2
    x_low = lon // 8
    x_all = (lat % 2) * 2 + x_low
    at_y = [((y + d) % 4) * 2 for d in range(4)]
    at_x = [(x_all + d) % 4 for d in range(4)]
    at_x = [(v // 2, (v % 2) * 8) for v in at_x]
    at_low = [((x_low + d) % 2) * 8 for d in range(2)]
    at_z = [((z + d) % 4) * 2 for d in range(4)]
    at_core = [core, 1 - core]
    everyone = [(at_y[dy] + at_x[dx][0], at_x[dx][1] + at_z[dz] + at_core[dc]) for dy, dx, dz, dc in FAR]
    row_peers = [at_low[dx] + at_z[dz] + at_core[dc] for dx, dz, dc in FAR_LON]

    def place(a, b):
        p = a * LON + b
        return jnp.where(a < LAT // 2, p, DEV + HALF - 1 - p)

    greeted = [(lat, b) for b in row_peers]
    x_high = lat % 2
    same, mirror = lon, (1 - x_low) * 8 + z * 2 + core
    greeted += [(at_y[d] + 1 - x_high, mirror) for d in (2, 1, 3, 0)] + [(at_y[d] + x_high, same) for d in (2, 1, 3)]
    for a, b in greeted:
        pl.semaphore_signal(barrier, inc=1, device_id={"lat": a, "lon": b})

    resp_ref[...] = jnp.zeros((8, 128), f32)
    for load in loads[1:]:
        load.start()
    loads[0].wait()

    def stage(block, carry):
        for r in range(ROWS):
            source = jnp.where(south == 1, ROWS - 1 - r, r)
            line = h_ref[pl.ds(ROWS * block + source, 1), :]
            send_a[block, 0, r] = line[:, :128]
            send_a[block, 1, r] = line[:, 128:]
        return carry

    lax.fori_loop(0, LON, stage, 0)

    for i in range(SLOTS):
        def coefficients(block, carry, i=i):
            row = block * 32
            m = (DEV * i + me).astype(f32)
            k = (row + lax.broadcasted_iota(jnp.int32, (32, 128), 0)).astype(f32)
            k1 = k + 1.0
            l2 = 2.0 * (m + k1)
            squared = (l2 * l2 - 1.0) / (k1 * (2.0 * m + k1))
            below = l2 - 2.0
            ratio = k * (2.0 * m + k) / jnp.maximum(below * below - 1.0, 1.0)
            start = pl.multiple_of(STARTS[i] + row, 8)
            coef_a[pl.ds(start, 32), :] = jnp.sqrt(squared)
            coef_c[pl.ds(start, 32), :] = jnp.sqrt(squared * ratio)
            return carry

        lax.fori_loop(0, (MODES - DEV * i) // 32, coefficients, 0)

    pl.semaphore_wait(barrier, len(greeted))

    def exchange_lon(send, recv, which):
        for b in row_peers:
            pltpu.make_async_remote_copy(
                send.at[b], recv.at[lon], ssem.at[which], rsem.at[which], device_id={"lat": lat, "lon": b}
            ).start()
        recv[lon] = send[lon]

    def finish(send, recv, which, count):
        every = pltpu.make_async_remote_copy(
            send.at[pl.ds(0, count)], recv.at[pl.ds(0, count)], ssem.at[which], rsem.at[which],
            device_id={"lat": lat, "lon": row_peers[0]},
        )
        every.wait_send()
        every.wait_recv()

    exchange_lon(send_a, recv_a, 0)

    loads[1].wait()
    x = geo_ref[0:8, :]
    starts = pltpu.roll(geo_ref[32:40, :], lax.rem(DEV - me, DEV), axis=1)
    state = []
    for i in range(SLOTS):
        m = (DEV * i + me).astype(f32)
        coarse = m * geo_ref[8:16, :]
        fine = m * geo_ref[16:24, :] + jnp.broadcast_to(starts[i : i + 1, 0:1], (8, 128))
        count = jnp.maximum(jnp.ceil((-84.0 - (coarse + fine)) * (1.0 / 64.0)), 0.0)
        value = jnp.exp2((coarse + 64.0 * count) + fine) * geo_ref[24:32, :]
        state.append((jnp.zeros_like(value), value, count))

    for section in range(SLOTS):
        active = SLOTS - section

        def steps(block, carry, section=section, active=active):
            new = []
            for i in range(active):
                earlier, latest, count = carry[i]
                base = STARTS[i] + section * DEV
                row = pl.multiple_of(base + block * 8, 8)
                a8 = coef_a[pl.ds(row, 8), :]
                c8 = coef_c[pl.ds(row, 8), :]
                seen = jnp.where(count == 0.0, 1.0, 0.0)
                for u in range(8):
                    tall[pl.ds(pl.multiple_of((row + u) * 8, 8), 8), :] = latest * seen
                    following = (a8[u : u + 1, :] * x) * latest - c8[u : u + 1, :] * earlier
                    earlier, latest = latest, following
                large = jnp.logical_and(jnp.abs(latest) > 2.0**-20, count > 0.0)
                factor = jnp.where(large, 2.0**-64, 1.0)
                new.append((earlier * factor, latest * factor, count - jnp.where(large, 1.0, 0.0)))
            return tuple(new)

        state = list(lax.fori_loop(0, DEV // 8, steps, tuple(state[:active])))

    loads[3].wait()
    thi_ref[...], tlo_ref[...] = split(table_ref[...])
    loads[2].wait()
    for side in range(2):
        lanes = slice(side * 128, side * 128 + 128)
        if side == 0:
            finish(send_a, recv_a, 0, LON - 1)
        d = [recv_a[b, side, :, 0, :] for b in range(LON)]
        even = {b: d[b] + d[16 - b] for b in range(1, 8)}
        odd = {b: d[b] - d[16 - b] for b in range(1, 8)}
        real = [None] * 9
        imag = [None] * 9
        for rho in range(5):
            a = combine(
                [(d[0], 1.0), (d[8], 1.0 - 2.0 * (rho % 2))] + [(even[b], cosine(rho * b)) for b in (2, 4, 6)]
            )
            b_ = combine([(even[b], cosine(rho * b)) for b in (1, 3, 5, 7)])
            e = combine([(odd[b], -sine(rho * b)) for b in (2, 4, 6)])
            c = combine([(odd[b], -sine(rho * b)) for b in (1, 3, 5, 7)])
            real[rho], real[8 - rho] = a + b_, a - b_
            imag[rho], imag[8 - rho] = c + e, c - e
        for rho in range(LON):
            tc = tw_ref[side * LON + rho : side * LON + rho + 1, :]
            ts = tw_ref[(2 + side) * LON + rho : (2 + side) * LON + rho + 1, :]
            if rho % 8 == 0:
                zre, zim = real[rho] * tc, -(real[rho] * ts)
            elif rho < 8:
                zre, zim = real[rho] * tc + imag[rho] * ts, imag[rho] * tc - real[rho] * ts
            else:
                yre, yim = real[16 - rho], imag[16 - rho]
                zre, zim = yre * tc - yim * ts, -(yim * tc) - yre * ts
            zs[rho, 0:ROWS, lanes] = zre
            zs[rho, 0:ROWS, CELLS + side * 128 : CELLS + side * 128 + 128] = zim

    zh, zl = split(zs[...].reshape(LON * 16, 2 * CELLS))
    thi, tlo = thi_ref[...], tlo_ref[...]
    nn = (((1,), (0,)), ((), ()))
    nt = (((1,), (1,)), ((), ()))

    def product(high, low, other_high, other_low, dims):
        count = high.shape[0]
        both = lax.dot_general(jnp.concatenate([high, low], axis=0), other_high, dims, preferred_element_type=f32)
        return both[:count] + both[count:] + lax.dot_general(high, other_low, dims, preferred_element_type=f32)

    osc[0 : LON * 16, :] = product(zh, zl, thi, tlo, nn)

    lane = lax.broadcasted_iota(jnp.int32, (LON, 128), 1)
    packed = [jnp.zeros((LON, 128), f32) for _ in range(LAT)]
    for r in range(ROWS):
        value = osc[pl.ds(r, LON, stride=16), :]
        mine = jnp.logical_and(lane >= 10 * r, lane < 10 * r + 10)
        for g in range(LAT):
            shift = (10 * (r - g)) % 128
            moved = pltpu.roll(value, shift, axis=1) if shift else value
            packed[g] = jnp.where(mine, moved, packed[g])
    for g in range(LAT):
        send_b[g * LON : (g + 1) * LON, :] = packed[g]

    def exchange_all(send, recv, which, source, target):
        for a, b in everyone:
            pltpu.make_async_remote_copy(
                send.at[pl.ds(source(a, b), 1)], recv.at[pl.ds(target, 1)], ssem.at[which], rsem.at[which],
                device_id={"lat": a, "lon": b},
            ).start()
        recv[pl.ds(target, 1), :] = send[pl.ds(source(lat, lon), 1), :]

    exchange_all(send_b, recv_b, 2, lambda a, b: a * LON + b, place(lat, lon))

    def halves(block, carry):
        row = pl.multiple_of(block * 128, 128)
        for j in range(5):
            value = tall[pl.ds(row * 8 + j, 128, stride=8), :]
            high, low = split(value)
            phi[pl.ds(row, 128), j * 128 : (j + 1) * 128] = high
            plo[pl.ds(row, 128), j * 128 : (j + 1) * 128] = low
            high, low = high.T, low.T
            phi_t[j * 128 : (j + 1) * 128, pl.ds(row, 128)] = high
            plo_t[j * 128 : (j + 1) * 128, pl.ds(row, 128)] = low
        return carry

    lax.fori_loop(0, TALL // 128, halves, 0)

    loads[4].wait()
    loads[5].wait()
    turned = pltpu.roll(resp_ref[...], lax.rem(DEV - me, DEV), axis=1)
    within = lax.broadcasted_iota(jnp.int32, (SLOTS, 128), 1) < DEV - me
    shifted = jnp.where(within, turned[0:SLOTS], turned[1 : SLOTS + 1])
    response = jnp.concatenate(
        [shifted[q : q + 1] for i in range(SLOTS) for q in range(i, SLOTS)], axis=1
    )
    first = jnp.where(jnp.logical_and(lax.broadcasted_iota(jnp.int32, (1, TALL), 1) < MODES, me == 0), 1.0, 2.0)
    response = response * first
    row = lax.broadcasted_iota(jnp.int32, (32, TALL), 0)
    column = lax.broadcasted_iota(jnp.int32, (32, TALL), 1)
    slot = jnp.zeros((32, TALL), jnp.int32)
    for i in range(1, SLOTS):
        slot = slot + jnp.where(column >= STARTS[i], 1, 0)
    wanted = 2 * slot + 16 * (column & 1)
    keep = jnp.logical_or(row == wanted, row == wanted + 1)
    gain = jnp.where(keep, response, 0.0)

    finish(send_b, recv_b, 2, DEV - 1)

    north = recv_b[0:HALF, :]
    southern = recv_b[HALF:DEV, :]
    weights = wt_ref[...]
    folded = jnp.concatenate([(north + southern) * weights, (north - southern) * weights], axis=0)
    fold[...] = folded.T
    left = lax.broadcasted_iota(jnp.int32, (10, 128), 1) < HALF
    evens = []
    odds = []
    for j in range(5):
        first_row = fold[20 * j : 20 * j + 10, :]
        if j < 4:
            second_row = fold[20 * j + 10 : 20 * j + 20, :]
        else:
            second_row = jnp.zeros((10, 128), f32)
        evens.append(jnp.where(left, first_row, pltpu.roll(second_row, HALF, axis=1)))
        odds.append(jnp.where(left, pltpu.roll(first_row, HALF, axis=1), second_row))
    pad = jnp.zeros((6, WIDE), f32)
    lhs = jnp.concatenate([jnp.concatenate(evens, axis=1), pad, jnp.concatenate(odds, axis=1), pad], axis=0)
    lh, ll = split(lhs)
    used = ROWS * HALF
    sh, sl = split(product(lh[:, :used], ll[:, :used], phi_t[:used], plo_t[:used], nn) * gain)
    synthesis = product(sh, sl, phi[...], plo[...], nn)
    fold[...] = jnp.zeros((128, 128), f32)
    for j in range(5):
        e = synthesis[0:10, j * 128 : (j + 1) * 128]
        o = synthesis[16:26, j * 128 : (j + 1) * 128]
        n, s = e + o, e - o
        fold[20 * j : 20 * j + 10, :] = jnp.where(left, n, pltpu.roll(s, HALF, axis=1))
        if j < 4:
            fold[20 * j + 10 : 20 * j + 20, :] = jnp.where(left, pltpu.roll(n, HALF, axis=1), s)
    send_c[...] = fold[...].T

    exchange_all(send_c, recv_c, 3, place, me)
    finish(send_c, recv_c, 3, DEV - 1)

    pieces = [recv_c[g * LON : (g + 1) * LON, :] for g in range(LAT)]
    gathered = []
    for r in range(ROWS):
        value = jnp.zeros((LON, 128), f32)
        for g in range(LAT):
            mine = jnp.logical_and(lane >= 10 * g, lane < 10 * g + 10)
            shift = (10 * (g - r)) % 128
            moved = pltpu.roll(pieces[g], shift, axis=1) if shift else pieces[g]
            value = jnp.where(mine, moved, value)
        gathered.append(value)
    gh, gl = split(jnp.concatenate(gathered, axis=0))
    inverse = product(gh, gl, thi, tlo, nt)
    for c in range(4):
        vs[c, 0 : ROWS * LON, :] = inverse[:, c * 128 : (c + 1) * 128]

    for side in range(2):
        lanes = slice(side * 128, side * 128 + 128)
        real = []
        imag = []
        for rho in range(LON):
            tc = tw_ref[side * LON + rho : side * LON + rho + 1, :]
            ts = tw_ref[(2 + side) * LON + rho : (2 + side) * LON + rho + 1, :]
            vre = vs[side, pl.ds(rho, ROWS, stride=16), :]
            vim = vs[2 + side, pl.ds(rho, ROWS, stride=16), :]
            real.append(vre * tc - vim * ts)
            imag.append(None if rho % 8 == 0 else vre * ts + vim * tc)
        ure = {rho: real[rho] + real[16 - rho] for rho in range(1, 8)}
        uim = {rho: imag[rho] - imag[16 - rho] for rho in range(1, 8)}
        def put(b, value, side=side):
            for r in range(ROWS):
                target = ROWS * b + jnp.where(south == 1, ROWS - 1 - r, r)
                send_d[side, pl.ds(target, 1), :] = value[r : r + 1]

        for b in range(5):
            ge = combine(
                [(real[0], 1.0), (real[8], 1.0 - 2.0 * (b % 2))] + [(ure[q], cosine(q * b)) for q in (2, 4, 6)]
            )
            go = combine([(ure[q], cosine(q * b)) for q in (1, 3, 5, 7)])
            he = combine([(uim[q], sine(q * b)) for q in (2, 4, 6)])
            ho = combine([(uim[q], sine(q * b)) for q in (1, 3, 5, 7)])
            put(b, (ge + go) - (he + ho))
            if b > 0:
                put(16 - b, (ge + go) + (he + ho))
            if b < 4:
                put(8 - b, (ge - go) - (ho - he))
                if b > 0:
                    put(8 + b, (ge - go) + (ho - he))
        for b in row_peers:
            pltpu.make_async_remote_copy(
                send_d.at[side, pl.ds(ROWS * b, ROWS)], recv_d.at[side, pl.ds(ROWS * lon, ROWS)],
                ssem.at[4 + side], rsem.at[4 + side], device_id={"lat": lat, "lon": b},
            ).start()
        for r in range(ROWS):
            recv_d[side, pl.ds(ROWS * lon + r, 1), :] = send_d[side, pl.ds(ROWS * lon + r, 1), :]

    for side in range(2):
        lanes = slice(side * 128, side * 128 + 128)
        finish(send_d.at[side], recv_d.at[side], 4 + side, ROWS * (LON - 1))
        o_ref[:, lanes] = recv_d[side]


def shards(height, response):
    fixed = constants()
    hbm = pl.BlockSpec(memory_space=pltpu.HBM)
    blocks = pltpu.VMEM((LON, 2, ROWS, 1, 128), f32)
    rows = pltpu.VMEM((DEV, 128), f32)
    out = pl.pallas_call(
        kernel,
        out_shape=jax.ShapeDtypeStruct((NLAT // LAT, CELLS), f32),
        in_specs=[hbm] * 3,
        out_specs=pl.BlockSpec(memory_space=pltpu.VMEM),
        scratch_shapes=[
            pltpu.VMEM((NLAT // LAT, CELLS), f32),
            pltpu.VMEM((8, 128), f32),
            pltpu.VMEM((2 * CELLS, 128), f32),
            pltpu.VMEM((2 * CELLS, 128), bf16),
            pltpu.VMEM((2 * CELLS, 128), bf16),
            pltpu.VMEM((4 * LON, 128), f32),
            pltpu.VMEM((40, 128), f32),
            pltpu.VMEM((HALF, 128), f32),
            blocks,
            blocks,
            pltpu.VMEM((LON, 16, 2 * CELLS), f32),
            pltpu.VMEM((LON * 16 + 16, 128), f32),
            rows,
            rows,
            pltpu.VMEM((TALL, 128), f32),
            pltpu.VMEM((TALL, 128), f32),
            pltpu.VMEM((TALL * 8 + 8, 128), f32),
            pltpu.VMEM((TALL, WIDE), bf16),
            pltpu.VMEM((TALL, WIDE), bf16),
            pltpu.VMEM((WIDE, TALL), bf16),
            pltpu.VMEM((WIDE, TALL), bf16),
            pltpu.VMEM((128, 128), f32),
            rows,
            rows,
            pltpu.VMEM((4, 16 * LON + 16, 128), f32),
            pltpu.VMEM((2, NLAT // LAT, 128), f32),
            pltpu.VMEM((2, NLAT // LAT, 128), f32),
            pltpu.SemaphoreType.DMA((6,)),
            pltpu.SemaphoreType.DMA((6,)),
            pltpu.SemaphoreType.DMA((6,)),
        ],
        compiler_params=pltpu.CompilerParams(
            collective_id=0, has_side_effects=True, vmem_limit_bytes=40 * 1024 * 1024
        ),
    )(
        pltpu.with_memory_space_constraint(height.reshape(NLAT // LAT, CELLS), pltpu.HBM),
        pltpu.with_memory_space_constraint(response.reshape(SLOTS, 128), pltpu.HBM),
        pltpu.with_memory_space_constraint(jnp.asarray(fixed), pltpu.HBM),
    )
    return out.reshape(height.shape)


def solution(mesh):
    placed = (P(None, "lat", "lon"), P())
    return jax.shard_map(
        shards, mesh=mesh, in_specs=placed, out_specs=P(None, "lat", "lon"), check_vma=False
    )
```

```python
import math

import jax
import jax.numpy as jnp
import numpy as np
from jax import lax
from jax.experimental import pallas as pl
from jax.experimental.pallas import tpu as pltpu
from jax.sharding import PartitionSpec as P

NLAT = 1152
NLON = 4096
MODES = 640
LON = 16
LAT = 8
DEV = LON * LAT
ROWS = NLAT // DEV
CELLS = NLON // LON
SLOTS = MODES // DEV
HALF = DEV // 2
STARTS = [sum(MODES - DEV * t for t in range(i)) for i in range(SLOTS)]
TALL = sum(MODES - DEV * t for t in range(SLOTS))
WIDE = 640
HOPS = (0, 1, 2, 1)
FAR = sorted(
    [(dy, dx, dz, dc) for dy in range(4) for dx in range(4) for dz in range(4) for dc in range(2)],
    key=lambda o: (-HOPS[o[0]] - HOPS[o[1]] - HOPS[o[2]], -o[3]),
)[: DEV - 1]
FAR_LON = sorted(
    [(dx, dz, dc) for dx in range(2) for dz in range(4) for dc in range(2)],
    key=lambda o: (-o[0] - HOPS[o[1]], -o[2]),
)[: LON - 1]
bf16 = jnp.bfloat16
f32 = jnp.float32


def constants():
    t = np.arange(CELLS)
    table = np.zeros((2 * CELLS, 128))
    for g in range(LAT):
        for i in range(SLOTS):
            angle = 2 * np.pi * ((g + LAT * i) * t % CELLS) / CELLS
            column = (g * SLOTS + i) * 2
            table[:CELLS, column] = np.cos(angle)
            table[CELLS:, column] = np.sin(angle)
            table[:CELLS, column + 1] = -np.sin(angle)
            table[CELLS:, column + 1] = np.cos(angle)
    angle = 2 * np.pi * np.arange(LON)[:, None] * t[None, :] / NLON
    twiddle = np.stack([np.cos(angle), np.sin(angle)]).astype(np.float32)
    geometry = np.zeros((5, 8, 128), np.float32)
    for chunk in range(5):
        for lane in range(128):
            r = 2 * chunk + lane // HALF
            if r < ROWS:
                theta = np.pi * (ROWS * (lane % HALF) + r + 0.5) / NLAT
                log_sine = np.log2(np.sin(theta))
                coarse = np.round(log_sine * 1024) / 1024
                geometry[:4, chunk, lane] = np.cos(theta), coarse, log_sine - coarse, 1.0
    weights = np.zeros((HALF, 128), np.float32)
    for r in range(ROWS):
        theta = np.pi * (ROWS * np.arange(HALF) + r + 0.5) / NLAT
        cell = np.sin(theta) * (np.pi / NLAT) * (2 * np.pi / NLON)
        weights[:, 10 * r : 10 * r + 10] = cell[:, None]
    first = [
        (0.5 * (math.lgamma(m + 1.5) - math.lgamma(1.5) - math.lgamma(m + 1.0)) - 0.5 * math.log(4 * math.pi))
        / math.log(2)
        for m in range(MODES)
    ]
    geometry[4, :SLOTS] = np.reshape(first, (SLOTS, DEV))
    twiddle = twiddle.reshape(2, LON, 2, 128).transpose(0, 2, 1, 3).reshape(4 * LON, 128)
    parts = [table.astype(np.float32), twiddle, geometry.reshape(40, 128), weights]
    return np.concatenate(parts)


def split(x):
    high = x.astype(bf16)
    return high, (x - high.astype(f32)).astype(bf16)


def cosine(n):
    return math.cos(math.pi * (n % 16) / 8)


def sine(n):
    return math.sin(math.pi * (n % 16) / 8)


def combine(terms):
    total = None
    for value, factor in terms:
        if abs(factor) < 1e-9:
            continue
        if abs(factor - 1) < 1e-9:
            term, negative = value, False
        elif abs(factor + 1) < 1e-9:
            term, negative = value, True
        else:
            term, negative = value * factor, False
        if total is None:
            total = -term if negative else term
        else:
            total = total - term if negative else total + term
    return 0.0 if total is None else total


def kernel(
    h_hbm, resp_hbm, fixed_hbm, o_ref,
    h_ref, resp_ref, table_ref, thi_ref, tlo_ref, tw_ref, geo_ref, wt_ref,
    send_a, recv_a, zs, osc, send_b, recv_b, coef_a, coef_c, tall, phi, plo, phi_t, plo_t, fold, send_c, recv_c, vs, send_d, recv_d,
    ssem, rsem, lsem,
):
    loads = [
        pltpu.make_async_copy(source, target, lsem.at[n])
        for n, (source, target) in enumerate(
            [
                (h_hbm, h_ref),
                (fixed_hbm.at[pl.ds(576, 40)], geo_ref),
                (fixed_hbm.at[pl.ds(512, 64)], tw_ref),
                (fixed_hbm.at[pl.ds(0, 512)], table_ref),
                (fixed_hbm.at[pl.ds(616, 64)], wt_ref),
                (resp_hbm, resp_ref.at[pl.ds(0, SLOTS)]),
            ]
        )
    ]
    loads[0].start()
    lon = lax.axis_index("lon")
    lat = lax.axis_index("lat")
    me = lat * LON + lon
    south = lat // (LAT // 2)
    barrier = pltpu.get_barrier_semaphore()

    y, z, core = lat // 2, (lon // 2) % 4, lon % 2
    x_low = lon // 8
    x_all = (lat % 2) * 2 + x_low
    at_y = [((y + d) % 4) * 2 for d in range(4)]
    at_x = [(x_all + d) % 4 for d in range(4)]
    at_x = [(v // 2, (v % 2) * 8) for v in at_x]
    at_low = [((x_low + d) % 2) * 8 for d in range(2)]
    at_z = [((z + d) % 4) * 2 for d in range(4)]
    at_core = [core, 1 - core]
    everyone = [(at_y[dy] + at_x[dx][0], at_x[dx][1] + at_z[dz] + at_core[dc]) for dy, dx, dz, dc in FAR]
    row_peers = [at_low[dx] + at_z[dz] + at_core[dc] for dx, dz, dc in FAR_LON]

    def place(a, b):
        p = a * LON + b
        return jnp.where(a < LAT // 2, p, DEV + HALF - 1 - p)

    greeted = [(lat, b) for b in row_peers]
    x_high = lat % 2
    same, mirror = lon, (1 - x_low) * 8 + z * 2 + core
    greeted += [(at_y[d] + 1 - x_high, mirror) for d in (2, 1, 3, 0)] + [(at_y[d] + x_high, same) for d in (2, 1, 3)]
    for a, b in greeted:
        pl.semaphore_signal(barrier, inc=1, device_id={"lat": a, "lon": b})

    resp_ref[...] = jnp.zeros((8, 128), f32)
    for load in loads[1:]:
        load.start()
    loads[0].wait()

    def stage(block, carry):
        for r in range(ROWS):
            source = jnp.where(south == 1, ROWS - 1 - r, r)
            line = h_ref[pl.ds(ROWS * block + source, 1), :]
            send_a[0, block, r] = line[:, :128]
            send_a[1, block, r] = line[:, 128:]
        return carry

    lax.fori_loop(0, LON, stage, 0)

    for i in range(SLOTS):
        def coefficients(block, carry, i=i):
            row = block * 32
            m = (DEV * i + me).astype(f32)
            k = (row + lax.broadcasted_iota(jnp.int32, (32, 128), 0)).astype(f32)
            k1 = k + 1.0
            l2 = 2.0 * (m + k1)
            squared = (l2 * l2 - 1.0) / (k1 * (2.0 * m + k1))
            below = l2 - 2.0
            ratio = k * (2.0 * m + k) / jnp.maximum(below * below - 1.0, 1.0)
            start = pl.multiple_of(STARTS[i] + row, 8)
            coef_a[pl.ds(start, 32), :] = jnp.sqrt(squared)
            coef_c[pl.ds(start, 32), :] = jnp.sqrt(squared * ratio)
            return carry

        lax.fori_loop(0, (MODES - DEV * i) // 32, coefficients, 0)

    pl.semaphore_wait(barrier, len(greeted))

    def exchange_lon(send, recv, which):
        for b in row_peers:
            pltpu.make_async_remote_copy(
                send.at[b], recv.at[lon], ssem.at[which], rsem.at[which], device_id={"lat": lat, "lon": b}
            ).start()
        recv[lon] = send[lon]

    def finish(send, recv, which, count):
        every = pltpu.make_async_remote_copy(
            send.at[pl.ds(0, count)], recv.at[pl.ds(0, count)], ssem.at[which], rsem.at[which],
            device_id={"lat": lat, "lon": row_peers[0]},
        )
        every.wait_send()
        every.wait_recv()

    for side in range(2):
        exchange_lon(send_a.at[side], recv_a.at[side], side)

    loads[1].wait()
    x = geo_ref[0:8, :]
    starts = pltpu.roll(geo_ref[32:40, :], lax.rem(DEV - me, DEV), axis=1)
    state = []
    for i in range(SLOTS):
        m = (DEV * i + me).astype(f32)
        coarse = m * geo_ref[8:16, :]
        fine = m * geo_ref[16:24, :] + jnp.broadcast_to(starts[i : i + 1, 0:1], (8, 128))
        count = jnp.maximum(jnp.ceil((-84.0 - (coarse + fine)) * (1.0 / 64.0)), 0.0)
        value = jnp.exp2((coarse + 64.0 * count) + fine) * geo_ref[24:32, :]
        state.append((jnp.zeros_like(value), value, count))

    for section in range(SLOTS):
        active = SLOTS - section

        def steps(block, carry, section=section, active=active):
            new = []
            for i in range(active):
                earlier, latest, count = carry[i]
                base = STARTS[i] + section * DEV
                row = pl.multiple_of(base + block * 8, 8)
                a8 = coef_a[pl.ds(row, 8), :]
                c8 = coef_c[pl.ds(row, 8), :]
                seen = jnp.where(count == 0.0, 1.0, 0.0)
                for u in range(8):
                    tall[pl.ds(pl.multiple_of((row + u) * 8, 8), 8), :] = latest * seen
                    following = (a8[u : u + 1, :] * x) * latest - c8[u : u + 1, :] * earlier
                    earlier, latest = latest, following
                large = jnp.logical_and(jnp.abs(latest) > 2.0**-20, count > 0.0)
                factor = jnp.where(large, 2.0**-64, 1.0)
                new.append((earlier * factor, latest * factor, count - jnp.where(large, 1.0, 0.0)))
            return tuple(new)

        state = list(lax.fori_loop(0, DEV // 8, steps, tuple(state[:active])))

    loads[3].wait()
    thi_ref[...], tlo_ref[...] = split(table_ref[...])
    loads[2].wait()
    for side in range(2):
        lanes = slice(side * 128, side * 128 + 128)
        finish(send_a.at[side], recv_a.at[side], side, LON - 1)
        d = [recv_a[side, b, :, 0, :] for b in range(LON)]
        even = {b: d[b] + d[16 - b] for b in range(1, 8)}
        odd = {b: d[b] - d[16 - b] for b in range(1, 8)}
        real = [None] * 9
        imag = [None] * 9
        for rho in range(5):
            a = combine(
                [(d[0], 1.0), (d[8], 1.0 - 2.0 * (rho % 2))] + [(even[b], cosine(rho * b)) for b in (2, 4, 6)]
            )
            b_ = combine([(even[b], cosine(rho * b)) for b in (1, 3, 5, 7)])
            e = combine([(odd[b], -sine(rho * b)) for b in (2, 4, 6)])
            c = combine([(odd[b], -sine(rho * b)) for b in (1, 3, 5, 7)])
            real[rho], real[8 - rho] = a + b_, a - b_
            imag[rho], imag[8 - rho] = c + e, c - e
        for rho in range(LON):
            tc = tw_ref[side * LON + rho : side * LON + rho + 1, :]
            ts = tw_ref[(2 + side) * LON + rho : (2 + side) * LON + rho + 1, :]
            if rho % 8 == 0:
                zre, zim = real[rho] * tc, -(real[rho] * ts)
            elif rho < 8:
                zre, zim = real[rho] * tc + imag[rho] * ts, imag[rho] * tc - real[rho] * ts
            else:
                yre, yim = real[16 - rho], imag[16 - rho]
                zre, zim = yre * tc - yim * ts, -(yim * tc) - yre * ts
            mine = slice(rho * ROWS, rho * ROWS + ROWS)
            zs[mine, lanes] = zre
            zs[mine, CELLS + side * 128 : CELLS + side * 128 + 128] = zim

    zh, zl = split(zs[...])
    thi, tlo = thi_ref[...], tlo_ref[...]
    nn = (((1,), (0,)), ((), ()))
    nt = (((1,), (1,)), ((), ()))

    def product(high, low, other_high, other_low, dims):
        count = high.shape[0]
        both = lax.dot_general(jnp.concatenate([high, low], axis=0), other_high, dims, preferred_element_type=f32)
        return both[:count] + both[count:] + lax.dot_general(high, other_low, dims, preferred_element_type=f32)

    osc[0 : LON * ROWS, :] = product(zh, zl, thi, tlo, nn)

    lane = lax.broadcasted_iota(jnp.int32, (LON, 128), 1)
    packed = [jnp.zeros((LON, 128), f32) for _ in range(LAT)]
    for r in range(ROWS):
        value = osc[pl.ds(r, LON, stride=ROWS), :]
        mine = jnp.logical_and(lane >= 10 * r, lane < 10 * r + 10)
        for g in range(LAT):
            shift = (10 * (r - g)) % 128
            moved = pltpu.roll(value, shift, axis=1) if shift else value
            packed[g] = jnp.where(mine, moved, packed[g])
    for g in range(LAT):
        send_b[g * LON : (g + 1) * LON, :] = packed[g]

    def exchange_all(send, recv, which, source, target):
        for a, b in everyone:
            pltpu.make_async_remote_copy(
                send.at[pl.ds(source(a, b), 1)], recv.at[pl.ds(target, 1)], ssem.at[which], rsem.at[which],
                device_id={"lat": a, "lon": b},
            ).start()
        recv[pl.ds(target, 1), :] = send[pl.ds(source(lat, lon), 1), :]

    exchange_all(send_b, recv_b, 2, lambda a, b: a * LON + b, place(lat, lon))

    def halves(block, carry):
        row = pl.multiple_of(block * 128, 128)
        for j in range(5):
            value = tall[pl.ds(row * 8 + j, 128, stride=8), :]
            high, low = split(value)
            phi[pl.ds(row, 128), j * 128 : (j + 1) * 128] = high
            plo[pl.ds(row, 128), j * 128 : (j + 1) * 128] = low
            high, low = high.T, low.T
            phi_t[j * 128 : (j + 1) * 128, pl.ds(row, 128)] = high
            plo_t[j * 128 : (j + 1) * 128, pl.ds(row, 128)] = low
        return carry

    lax.fori_loop(0, TALL // 128, halves, 0)

    loads[4].wait()
    loads[5].wait()
    turned = pltpu.roll(resp_ref[...], lax.rem(DEV - me, DEV), axis=1)
    within = lax.broadcasted_iota(jnp.int32, (SLOTS, 128), 1) < DEV - me
    shifted = jnp.where(within, turned[0:SLOTS], turned[1 : SLOTS + 1])
    response = jnp.concatenate(
        [shifted[q : q + 1] for i in range(SLOTS) for q in range(i, SLOTS)], axis=1
    )
    first = jnp.where(jnp.logical_and(lax.broadcasted_iota(jnp.int32, (1, TALL), 1) < MODES, me == 0), 1.0, 2.0)
    response = response * first
    row = lax.broadcasted_iota(jnp.int32, (32, TALL), 0)
    column = lax.broadcasted_iota(jnp.int32, (32, TALL), 1)
    slot = jnp.zeros((32, TALL), jnp.int32)
    for i in range(1, SLOTS):
        slot = slot + jnp.where(column >= STARTS[i], 1, 0)
    wanted = 2 * slot + 16 * (column & 1)
    keep = jnp.logical_or(row == wanted, row == wanted + 1)
    gain = jnp.where(keep, response, 0.0)

    finish(send_b, recv_b, 2, DEV - 1)

    north = recv_b[0:HALF, :]
    southern = recv_b[HALF:DEV, :]
    weights = wt_ref[...]
    folded = jnp.concatenate([(north + southern) * weights, (north - southern) * weights], axis=0)
    fold[...] = folded.T
    left = lax.broadcasted_iota(jnp.int32, (10, 128), 1) < HALF
    evens = []
    odds = []
    for j in range(5):
        first_row = fold[20 * j : 20 * j + 10, :]
        if j < 4:
            second_row = fold[20 * j + 10 : 20 * j + 20, :]
        else:
            second_row = jnp.zeros((10, 128), f32)
        evens.append(jnp.where(left, first_row, pltpu.roll(second_row, HALF, axis=1)))
        odds.append(jnp.where(left, pltpu.roll(first_row, HALF, axis=1), second_row))
    pad = jnp.zeros((6, WIDE), f32)
    lhs = jnp.concatenate([jnp.concatenate(evens, axis=1), pad, jnp.concatenate(odds, axis=1), pad], axis=0)
    lh, ll = split(lhs)
    used = ROWS * HALF
    sh, sl = split(product(lh[:, :used], ll[:, :used], phi_t[:used], plo_t[:used], nn) * gain)
    synthesis = product(sh, sl, phi[...], plo[...], nn)
    fold[...] = jnp.zeros((128, 128), f32)
    for j in range(5):
        e = synthesis[0:10, j * 128 : (j + 1) * 128]
        o = synthesis[16:26, j * 128 : (j + 1) * 128]
        n, s = e + o, e - o
        fold[20 * j : 20 * j + 10, :] = jnp.where(left, n, pltpu.roll(s, HALF, axis=1))
        if j < 4:
            fold[20 * j + 10 : 20 * j + 20, :] = jnp.where(left, pltpu.roll(n, HALF, axis=1), s)
    send_c[...] = fold[...].T

    exchange_all(send_c, recv_c, 3, place, me)
    finish(send_c, recv_c, 3, DEV - 1)

    pieces = [recv_c[g * LON : (g + 1) * LON, :] for g in range(LAT)]
    gathered = []
    for r in range(ROWS):
        value = jnp.zeros((LON, 128), f32)
        for g in range(LAT):
            mine = jnp.logical_and(lane >= 10 * g, lane < 10 * g + 10)
            shift = (10 * (g - r)) % 128
            moved = pltpu.roll(pieces[g], shift, axis=1) if shift else pieces[g]
            value = jnp.where(mine, moved, value)
        gathered.append(value)
    gh, gl = split(jnp.concatenate(gathered, axis=0))
    inverse = product(gh, gl, thi, tlo, nt)
    for c in range(4):
        vs[c, 0 : ROWS * LON, :] = inverse[:, c * 128 : (c + 1) * 128]

    for side in range(2):
        lanes = slice(side * 128, side * 128 + 128)
        real = []
        imag = []
        for rho in range(LON):
            tc = tw_ref[side * LON + rho : side * LON + rho + 1, :]
            ts = tw_ref[(2 + side) * LON + rho : (2 + side) * LON + rho + 1, :]
            vre = vs[side, pl.ds(rho, ROWS, stride=16), :]
            vim = vs[2 + side, pl.ds(rho, ROWS, stride=16), :]
            real.append(vre * tc - vim * ts)
            imag.append(None if rho % 8 == 0 else vre * ts + vim * tc)
        ure = {rho: real[rho] + real[16 - rho] for rho in range(1, 8)}
        uim = {rho: imag[rho] - imag[16 - rho] for rho in range(1, 8)}
        def put(b, value, side=side):
            for r in range(ROWS):
                target = ROWS * b + jnp.where(south == 1, ROWS - 1 - r, r)
                send_d[side, pl.ds(target, 1), :] = value[r : r + 1]

        for b in range(5):
            ge = combine(
                [(real[0], 1.0), (real[8], 1.0 - 2.0 * (b % 2))] + [(ure[q], cosine(q * b)) for q in (2, 4, 6)]
            )
            go = combine([(ure[q], cosine(q * b)) for q in (1, 3, 5, 7)])
            he = combine([(uim[q], sine(q * b)) for q in (2, 4, 6)])
            ho = combine([(uim[q], sine(q * b)) for q in (1, 3, 5, 7)])
            put(b, (ge + go) - (he + ho))
            if b > 0:
                put(16 - b, (ge + go) + (he + ho))
            if b < 4:
                put(8 - b, (ge - go) - (ho - he))
                if b > 0:
                    put(8 + b, (ge - go) + (ho - he))
        for b in row_peers:
            pltpu.make_async_remote_copy(
                send_d.at[side, pl.ds(ROWS * b, ROWS)], recv_d.at[side, pl.ds(ROWS * lon, ROWS)],
                ssem.at[4 + side], rsem.at[4 + side], device_id={"lat": lat, "lon": b},
            ).start()
        for r in range(ROWS):
            recv_d[side, pl.ds(ROWS * lon + r, 1), :] = send_d[side, pl.ds(ROWS * lon + r, 1), :]

    for side in range(2):
        lanes = slice(side * 128, side * 128 + 128)
        finish(send_d.at[side], recv_d.at[side], 4 + side, ROWS * (LON - 1))
        o_ref[:, lanes] = recv_d[side]


def shards(height, response):
    fixed = constants()
    hbm = pl.BlockSpec(memory_space=pltpu.HBM)
    blocks = pltpu.VMEM((2, LON, ROWS, 1, 128), f32)
    rows = pltpu.VMEM((DEV, 128), f32)
    out = pl.pallas_call(
        kernel,
        out_shape=jax.ShapeDtypeStruct((NLAT // LAT, CELLS), f32),
        in_specs=[hbm] * 3,
        out_specs=pl.BlockSpec(memory_space=pltpu.VMEM),
        scratch_shapes=[
            pltpu.VMEM((NLAT // LAT, CELLS), f32),
            pltpu.VMEM((8, 128), f32),
            pltpu.VMEM((2 * CELLS, 128), f32),
            pltpu.VMEM((2 * CELLS, 128), bf16),
            pltpu.VMEM((2 * CELLS, 128), bf16),
            pltpu.VMEM((4 * LON, 128), f32),
            pltpu.VMEM((40, 128), f32),
            pltpu.VMEM((HALF, 128), f32),
            blocks,
            blocks,
            pltpu.VMEM((LON * ROWS, 2 * CELLS), f32),
            pltpu.VMEM((LON * ROWS + 16, 128), f32),
            rows,
            rows,
            pltpu.VMEM((TALL, 128), f32),
            pltpu.VMEM((TALL, 128), f32),
            pltpu.VMEM((TALL * 8 + 8, 128), f32),
            pltpu.VMEM((TALL, WIDE), bf16),
            pltpu.VMEM((TALL, WIDE), bf16),
            pltpu.VMEM((WIDE, TALL), bf16),
            pltpu.VMEM((WIDE, TALL), bf16),
            pltpu.VMEM((128, 128), f32),
            rows,
            rows,
            pltpu.VMEM((4, 16 * LON + 16, 128), f32),
            pltpu.VMEM((2, NLAT // LAT, 128), f32),
            pltpu.VMEM((2, NLAT // LAT, 128), f32),
            pltpu.SemaphoreType.DMA((6,)),
            pltpu.SemaphoreType.DMA((6,)),
            pltpu.SemaphoreType.DMA((6,)),
        ],
        compiler_params=pltpu.CompilerParams(
            collective_id=0, has_side_effects=True, vmem_limit_bytes=40 * 1024 * 1024
        ),
    )(
        pltpu.with_memory_space_constraint(height.reshape(NLAT // LAT, CELLS), pltpu.HBM),
        pltpu.with_memory_space_constraint(response.reshape(SLOTS, 128), pltpu.HBM),
        pltpu.with_memory_space_constraint(jnp.asarray(fixed), pltpu.HBM),
    )
    return out.reshape(height.shape)


def solution(mesh):
    placed = (P(None, "lat", "lon"), P())
    return jax.shard_map(
        shards, mesh=mesh, in_specs=placed, out_specs=P(None, "lat", "lon"), check_vma=False
    )
```
